32 devices in a mesh: tm: 8 (over z, y), node: 4 (over x, core).
Axes of the slice: x: 2, y: 2, z: 4, core: 2. Of those that a mesh axis runs over, the one named last changes fastest.
Arguments:
- slice_starts: float32 [8, 32, 16384], P('tm'), may hold values from -1 to 1
- coupling: float32 [32, 16384], replicated, may hold values from 0.03 to 0.25
Outputs:
- node_values: float32 [8, 4, 32, 16384], P('tm', 'node')
- residual_log: float32 [3, 32], replicated
The draws below stay inside these ranges and needn't reach their ends.
All inputs are finite; a program needn't handle non-finite values.
Results may differ from the reference program's by a relative error of at most 0.0001.
Values sent between devices are 32-bit elements.
A program may use at most 128 MiB of HBM per device.

```python
import math
import jax
import jax.numpy as jnp
from jax import lax

X = 16384
SYS = 32
M = 4
SWEEPS = 3
NEWTON = 2
SLICES = 8


def block_scale(stream_key, shape, pieces, least, top_value):
    level, own = 1.0, jax.random.fold_in(stream_key, 6)
    for position, shards_of in pieces:
        draws = jnp.exp(jax.random.uniform(jax.random.fold_in(own, position), (shards_of,), jnp.float32, least / len(pieces), top_value / len(pieces)))
        level = level * jnp.repeat(draws, shape[position] // shards_of).reshape([-1 if axis == position else 1 for axis in range(len(shape))])
    return level


def setup_inputs(seed: int = 0) -> dict:
    key_of = jax.random.split(jax.random.key(seed), 3)
    return {
        "slice_starts": jnp.clip(jax.random.uniform(key_of[0], (SLICES, SYS, X), jnp.float32, -1.0, 1.0) * block_scale(key_of[0], (SLICES, SYS, X), ((0, 8),), -0.4, 0.0), -1.0, 1.0),
        "coupling": jnp.clip(jnp.exp(jax.random.uniform(key_of[1], (SYS, X), jnp.float32, math.log(0.03), math.log(0.25))), 0.03, 0.25),
    }


time_step = 0.5
log_floor = 0.05


def legendre_gap(point, node_count):
    before = 1.0
    current = point
    for degree in range(1, node_count):
        following = ((2 * degree + 1) * point * current - degree * before) / (degree + 1)
        before = current
        current = following
    return current - before


def collocation(node_count):
    points = []
    samples = 4000
    for sample_index in range(samples - 1):
        lower_end = -1.0 + 2.0 * sample_index / samples
        upper_end = -1.0 + 2.0 * (sample_index + 1) / samples
        lower_value = legendre_gap(lower_end, node_count)
        upper_value = legendre_gap(upper_end, node_count)
        if lower_value * upper_value < 0.0:
            for halving in range(80):
                middle = 0.5 * (lower_end + upper_end)
                middle_value = legendre_gap(middle, node_count)
                if lower_value * middle_value <= 0.0:
                    upper_end = middle
                else:
                    lower_end = middle
                    lower_value = middle_value
            points.append(0.5 * (lower_end + upper_end))
    points.append(1.0)
    node_times = [(point + 1.0) / 2.0 for point in points]
    matrix = [[0.0] * node_count for row_index in range(node_count)]
    for column in range(node_count):
        coeffs = [1.0]
        for other in range(node_count):
            if other != column:
                scale = node_times[column] - node_times[other]
                shifted = [0.0] + coeffs
                scaled = [value * node_times[other] for value in coeffs] + [0.0]
                coeffs = [(shifted[power] - scaled[power]) / scale for power in range(len(shifted))]
        for row_index in range(node_count):
            upper_time = node_times[row_index]
            matrix[row_index][column] = sum(coeffs[power] * upper_time ** (power + 1) / (power + 1) for power in range(len(coeffs)))
    return node_times, matrix


def operator_term(field_values, coupling):
    right_side = jnp.roll(field_values, -1, axis=-1)
    left_side = jnp.roll(field_values, 1, axis=-1)
    left_coupling = jnp.roll(coupling, 1, axis=-1)
    cubic = field_values * field_values * field_values
    return coupling * (right_side - field_values) - left_coupling * (field_values - left_side) + field_values - cubic


def reference(slice_starts, coupling):
    node_times, matrix = collocation(M)
    weights = jnp.asarray(matrix, jnp.float32)
    diag_weights = jnp.asarray([time_step * moment / M for moment in node_times], jnp.float32)
    implicit = diag_weights[None, :, None, None]
    node_state = jnp.broadcast_to(slice_starts[:, None], (SLICES, M, SYS, X))
    end_values = slice_starts
    residual_list = []
    for sweep_index in range(SWEEPS):
        starts = jnp.concatenate([slice_starts[:1], end_values[:-1]], axis=0)
        forcing = operator_term(node_state, coupling)
        quadrature = jnp.einsum("mj,pjsx->pmsx", weights, forcing, precision=lax.Precision.HIGHEST)
        base = starts[:, None] + time_step * quadrature
        defect = base - node_state
        mean_square = jnp.sum(defect * defect, axis=(0, 1, 3)) / (SLICES * M * X)
        residual_list.append(jnp.log(log_floor + mean_square))
        target = base - implicit * (node_state - node_state * node_state * node_state)
        iterate = node_state
        for newton_step in range(NEWTON):
            cubic = iterate * iterate * iterate
            derivative = 1.0 - implicit + 3.0 * implicit * iterate * iterate
            iterate = iterate - (iterate - implicit * (iterate - cubic) - target) / derivative
        node_state = iterate
        end_values = node_state[:, M - 1]
    return node_state, jnp.stack(residual_list)
```

```python
import functools
import jax
import jax.numpy as jnp
from jax import lax
from jax.experimental import pallas as pl
from jax.experimental.pallas import tpu as pltpu
from jax.sharding import PartitionSpec as P

M = 4
CHUNKS = 8
STEP = 8
LANE = 128
HALO = 3
PAD = 4
MESH = pl.DeviceIdType.MESH

time_step = 0.5
log_floor = 0.05


def legendre_gap(point, node_count):
    before = 1.0
    current = point
    for degree in range(1, node_count):
        following = ((2 * degree + 1) * point * current - degree * before) / (degree + 1)
        before = current
        current = following
    return current - before


def collocation(node_count):
    points = []
    samples = 4000
    for sample_index in range(samples - 1):
        lower_end = -1.0 + 2.0 * sample_index / samples
        upper_end = -1.0 + 2.0 * (sample_index + 1) / samples
        lower_value = legendre_gap(lower_end, node_count)
        upper_value = legendre_gap(upper_end, node_count)
        if lower_value * upper_value < 0.0:
            for halving in range(80):
                middle = 0.5 * (lower_end + upper_end)
                middle_value = legendre_gap(middle, node_count)
                if lower_value * middle_value <= 0.0:
                    upper_end = middle
                else:
                    lower_end = middle
                    lower_value = middle_value
            points.append(0.5 * (lower_end + upper_end))
    points.append(1.0)
    node_times = [(point + 1.0) / 2.0 for point in points]
    matrix = [[0.0] * node_count for row_index in range(node_count)]
    for column in range(node_count):
        coeffs = [1.0]
        for other in range(node_count):
            if other != column:
                scale = node_times[column] - node_times[other]
                shifted = [0.0] + coeffs
                scaled = [value * node_times[other] for value in coeffs] + [0.0]
                coeffs = [(shifted[power] - scaled[power]) / scale for power in range(len(shifted))]
        for row_index in range(node_count):
            upper_time = node_times[row_index]
            matrix[row_index][column] = sum(
                (
                    coeffs[power] * upper_time ** (power + 1) / (power + 1)
                    for power in range(len(coeffs))
                )
            )
    return (node_times, matrix)


def kernel(
    slices, rows, cells,
    start_hbm, coupling_hbm, out_hbm, log_ref,
    own, couple, prev1, prev2, prev3, here, there, mid, before, result,
    acc, part_tm, part_node,
    load_sem, s_prev1, r_prev1, s_prev2, r_prev2, s_prev3, r_prev3,
    s_out, r_out, local_sem, s_tm, r_tm, s_node, r_node,
):
    p = lax.axis_index("tm")
    n = lax.axis_index("node")
    chunk = cells // CHUNKS
    tiles = chunk // LANE
    all_tiles = cells // LANE
    my_rows = pl.ds(pl.multiple_of(n * rows, rows), rows)
    node_times, matrix = collocation(M)
    weight = [[time_step * value for value in line] for line in matrix]
    total = [sum(line) for line in weight]
    implicit = [time_step * moment / M for moment in node_times]
    even = lax.rem(p, 2) == 0
    first = p == 0
    second = p == 1

    loads = []
    for index, (source, target) in enumerate(
        ((start_hbm.at[0, my_rows], own), (coupling_hbm.at[my_rows], couple))
    ):
        for piece, (lo, to, size) in enumerate(
            ((0, PAD * LANE, cells), (cells - HALO * LANE, LANE, HALO * LANE), (0, PAD * LANE + cells, HALO * LANE))
        ):
            copy = pltpu.make_async_copy(
                source.at[:, pl.ds(lo, size)],
                target.at[:, pl.ds(to, size)],
                load_sem.at[index, piece],
            )
            copy.start()
            loads.append(copy)

    barrier = pltpu.get_barrier_semaphore()
    for step in range(1, slices):
        pl.semaphore_signal(
            barrier, inc=1, device_id={"tm": lax.rem(p + step, slices), "node": n}, device_id_type=MESH
        )
    for step in range(1, M):
        pl.semaphore_signal(
            barrier, inc=1, device_id={"tm": p, "node": lax.rem(n + step, M)}, device_id_type=MESH
        )
    pl.semaphore_wait(barrier, slices - 1 + M - 1)
    for copy in loads:
        copy.wait()

    def remote(source, target, send, recv, tm, node):
        return pltpu.make_async_remote_copy(
            src_ref=source, dst_ref=target, send_sem=send, recv_sem=recv,
            device_id={"tm": tm, "node": node}, device_id_type=MESH,
        )

    partner = jnp.where(even, p + 1, p - 1)
    ahead = lax.rem(p + 2, slices)

    def part(ref, c):
        begin = (c * tiles + HALO if c else -HALO) + PAD
        end = (c + 1) * tiles + HALO + PAD
        return ref.at[:, pl.ds(begin * LANE, (end - begin) * LANE)]

    def to_partner_own(c):
        return remote(part(own, c), part(prev1, c), s_prev1.at[c], r_prev1.at[c], partner, n)

    def to_partner_forward(c):
        return remote(part(prev2, c), part(prev1, c), s_prev1.at[c], r_prev1.at[c], partner, n)

    def ahead_own(c):
        return remote(part(own, c), part(prev2, c), s_prev2.at[c], r_prev2.at[c], ahead, n)

    def ahead_forward(c):
        return remote(part(prev1, c), part(prev3, c), s_prev3.at[c], r_prev3.at[c], ahead, n)

    has_behind = p >= 2
    has_ahead = p + 2 < slices
    odd = jnp.logical_not(even)

    def start_ahead(c):
        @pl.when(has_ahead)
        def _():
            ahead_own(c).start()

    @pl.when(even)
    def _():
        for c in range(CHUNKS):
            to_partner_own(c).start()
    def pass_across(c):
        @pl.when(has_behind)
        def _():
            ahead_own(c).wait_recv()

        @pl.when(jnp.logical_and(odd, has_behind))
        def _():
            to_partner_forward(c).start()

    def pass_ahead(c):
        @pl.when(odd)
        def _():
            to_partner_own(c).wait_recv()

        @pl.when(jnp.logical_and(even, has_behind))
        def _():
            to_partner_forward(c).wait_recv()

        @pl.when(jnp.logical_and(has_ahead, jnp.logical_not(first)))
        def _():
            ahead_forward(c).start()

    for c in range(3):
        start_ahead(c)

    acc[...] = jnp.zeros_like(acc)

    def diffusion(v, c, k):
        size = (k + 2) * LANE
        right = pltpu.roll(v, size - 1, 1)
        flux = c * (right - v)
        left = pltpu.roll(flux, 1, 1)
        return (flux - left)[:, LANE:LANE + k * LANE]

    def two_steps(base, u, square, reaction, a):
        s = (3.0 * a) * square - a
        d = 1.0 + s
        top = base + u * s
        target = base - a * reaction
        dd = d * d
        tt = top * top
        above = target * (d * dd) + (2.0 * a) * (top * tt)
        below = d * ((1.0 - a) * dd + (3.0 * a) * tt)
        guess = pl.reciprocal(below, approx=True)
        return above * (guess * (2.0 - below * guess))

    def folded(value, k):
        out = value[:, :LANE]
        for piece in range(1, k):
            out = out + value[:, piece * LANE:(piece + 1) * LANE]
        return out

    def run(begin, end, block, counted):
        count = (end - begin) // STEP

        def step(i, carry):
            block(begin + i * STEP, STEP, counted)
            return carry

        lax.fori_loop(0, count, step, 0)
        if begin + count * STEP < end:
            block(begin + count * STEP, end - begin - count * STEP, counted)

    def over(c, lag, block):
        begin = c * tiles + lag if c else 0
        end = min((c + 1) * tiles + lag, all_tiles)
        if c == 0 and lag:
            block(-lag, lag, False)
        run(begin, end, block, True)
        if c == CHUNKS - 1 and lag:
            block(all_tiles, lag, False)

    def lanes(offset):
        return offset * LANE if isinstance(offset, int) else pl.multiple_of(offset * LANE, LANE)

    def wide(tile, k):
        return pl.ds(lanes(tile + PAD - 1), (k + 2) * LANE)

    def centre(tile, k):
        return pl.ds(lanes(tile + PAD), k * LANE)

    pass_across(0)
    pass_across(1)
    pass_ahead(0)
    for c in range(CHUNKS):
        base_lane = c * chunk

        if c + 3 < CHUNKS:
            start_ahead(c + 3)
        if c + 1 < CHUNKS:
            pass_ahead(c + 1)

        @pl.when(p >= 3)
        def _():
            ahead_forward(c).wait_recv()

        def stage_a(tile, k, counted):
            mid_slice = slice(LANE, LANE + k * LANE)
            cw = couple[:, wide(tile, k)]
            at = centre(tile, k)
            vw = own[:, wide(tile, k)]
            v = vw[:, mid_slice]
            p1w = jnp.where(first, vw, prev1[:, wide(tile, k)])
            p1 = p1w[:, mid_slice]
            p2w = jnp.where(p <= 1, p1w, prev2[:, wide(tile, k)])
            p2 = p2w[:, mid_slice]
            p3 = jnp.where(p <= 2, p2, prev3[:, at])

            square = v * v
            reaction = v - v * square
            forcing = diffusion(vw, cw, k) + reaction
            found = None
            for m in range(M):
                base = p1 + total[m] * forcing
                if counted:
                    defect = base - v
                    found = defect * defect if found is None else found + defect * defect
                here[m, :, at] = two_steps(base, v, square, reaction, implicit[m])
            if counted:
                acc[0] += folded(found, k)

            square = p1 * p1
            reaction = p1 - p1 * square
            forcing = diffusion(p1w, cw, k) + reaction
            for m in range(M):
                there[m, :, at] = two_steps(p2 + total[m] * forcing, p1, square, reaction, implicit[m])

            square = p2 * p2
            reaction = p2 - p2 * square
            forcing = diffusion(p2w, cw, k) + reaction
            last = two_steps(
                p3 + total[M - 1] * forcing, p2, square, reaction, implicit[M - 1]
            )
            before[:, at] = jnp.where(second, p1, last)

        over(c, 2, stage_a)
        if c + 2 < CHUNKS:
            pass_across(c + 2)

        def update(source, begin, cw, tile, k, which, counted):
            values = []
            forcings = []
            for m in range(M):
                vw = source[m, :, wide(tile, k)]
                v = vw[:, LANE:LANE + k * LANE]
                square = v * v
                reaction = v - v * square
                values.append((v, square, reaction))
                forcings.append(diffusion(vw, cw, k) + reaction)
            found = None
            outputs = []
            for m in range(M):
                base = begin
                for j in range(M):
                    base = base + weight[m][j] * forcings[j]
                v, square, reaction = values[m]
                if counted:
                    defect = base - v
                    found = defect * defect if found is None else found + defect * defect
                outputs.append(two_steps(base, v, square, reaction, implicit[m]))
            if counted:
                acc[which] += folded(found, k)
            return outputs

        def stage_b(tile, k, counted):
            cw = couple[:, wide(tile, k)]
            at = centre(tile, k)
            begin = jnp.where(first, own[:, centre(tile, k)], there[M - 1, :, at])
            outputs = update(here, begin, cw, tile, k, 1, counted)
            for m in range(M):
                mid[m, :, at] = outputs[m]
            mixed = None
            mixed_reaction = None
            for m in range(M):
                w = weight[M - 1][m]
                vw = there[m, :, wide(tile, k)]
                v = vw[:, LANE:LANE + k * LANE]
                square = v * v
                reaction = v - v * square
                mixed = w * vw if mixed is None else mixed + w * vw
                mixed_reaction = w * reaction if mixed_reaction is None else mixed_reaction + w * reaction
            base = before[:, at] + (diffusion(mixed, cw, k) + mixed_reaction)
            last = two_steps(base, v, square, reaction, implicit[M - 1])
            before[:, at] = jnp.where(first, own[:, centre(tile, k)], last)

        over(c, 1, stage_b)

        def stage_c(tile, k, counted):
            cw = couple[:, wide(tile, k)]
            outputs = update(mid, before[:, centre(tile, k)], cw, tile, k, 2, counted)
            at = pl.ds(lanes(tile - c * tiles), k * LANE)
            for m in range(M):
                result[c, m, :, at] = outputs[m]

        over(c, 0, stage_c)

        target = out_hbm.at[0, 0, my_rows, pl.ds(base_lane, chunk)]
        for step in (2, 3, 1):
            peer = lax.rem(n + step, M)
            remote(result.at[c, peer], target, s_out.at[c, step], r_out.at[c, step], p, peer).start()
        pltpu.make_async_copy(result.at[c, n], target, local_sem.at[c]).start()

    lane = lax.broadcasted_iota(jnp.int32, (rows, LANE), 1)
    sub = lax.broadcasted_iota(jnp.int32, (rows, LANE), 0)
    place = lax.broadcasted_iota(jnp.int32, (8, LANE), 0)
    tile_value = jnp.zeros((8, LANE), jnp.float32)
    for which in range(3):
        per_system = jnp.sum(acc[which], axis=1, keepdims=True)
        row = jnp.sum(
            jnp.where(lane == n * rows + sub, per_system, 0.0), axis=0, keepdims=True
        )
        tile_value = tile_value + jnp.where(place == which, row, 0.0)
    part_tm[p] = tile_value
    sends = []
    for step in range(1, slices):
        copy = remote(
            part_tm.at[p], part_tm.at[p], s_tm.at[step], r_tm.at[step], lax.rem(p + step, slices), n
        )
        copy.start()
        sends.append(copy)
    for step in range(1, slices):
        source = lax.rem(p - step + slices, slices)
        remote(part_tm.at[source], part_tm.at[source], s_tm.at[step], r_tm.at[step], p, n).wait_recv()
    summed = part_tm[0]
    for index in range(1, slices):
        summed = summed + part_tm[index]
    part_node[n] = summed
    for step in range(1, M):
        copy = remote(
            part_node.at[n], part_node.at[n], s_node.at[step], r_node.at[step], p, lax.rem(n + step, M)
        )
        copy.start()
        sends.append(copy)
    for step in range(1, M):
        source = lax.rem(n - step + M, M)
        remote(part_node.at[source], part_node.at[source], s_node.at[step], r_node.at[step], p, n).wait_recv()
    summed = part_node[0]
    for index in range(1, M):
        summed = summed + part_node[index]
    log_ref[...] = jnp.log(log_floor + summed / (slices * M * cells))[:3, :M * rows]

    for copy in sends:
        copy.wait_send()
    for c in range(CHUNKS):
        here_rows = pl.ds(c * chunk, chunk)
        for step in range(1, M):
            source = lax.rem(n - step + M, M)
            landed = out_hbm.at[0, 0, pl.ds(pl.multiple_of(source * rows, rows), rows), here_rows]
            arrived = remote(result.at[c, n], landed, s_out.at[c, step], r_out.at[c, step], p, n)
            arrived.wait_recv()
            arrived.wait_send()
        pltpu.make_async_copy(result.at[c, n], out_hbm.at[0, 0, my_rows, here_rows], local_sem.at[c]).wait()

        @pl.when(has_ahead)
        def _():
            ahead_own(c).wait_send()

        @pl.when(jnp.logical_and(has_ahead, jnp.logical_not(first)))
        def _():
            ahead_forward(c).wait_send()

        @pl.when(even)
        def _():
            to_partner_own(c).wait_send()

        @pl.when(jnp.logical_and(odd, has_behind))
        def _():
            to_partner_forward(c).wait_send()


def solution(mesh):
    slices = mesh.shape["tm"]

    def body(slice_starts, coupling):
        systems, cells = coupling.shape
        rows = systems // M
        chunk = cells // CHUNKS
        padded = cells + 2 * PAD * LANE
        f32 = jnp.float32
        dma = pltpu.SemaphoreType.DMA
        anywhere = pl.BlockSpec(memory_space=pltpu.HBM)
        values, logs = pl.pallas_call(
            functools.partial(kernel, slices, rows, cells),
            out_shape=(
                jax.ShapeDtypeStruct((1, 1, systems, cells), f32),
                jax.ShapeDtypeStruct((3, systems), f32),
            ),
            in_specs=[anywhere, anywhere],
            out_specs=(pl.BlockSpec(memory_space=pl.ANY), pl.BlockSpec(memory_space=pltpu.VMEM)),
            scratch_shapes=[
                pltpu.VMEM((rows, padded), f32),
                pltpu.VMEM((rows, padded), f32),
                pltpu.VMEM((rows, padded), f32),
                pltpu.VMEM((rows, padded), f32),
                pltpu.VMEM((rows, padded), f32),
                pltpu.VMEM((M, rows, padded), f32),
                pltpu.VMEM((M, rows, padded), f32),
                pltpu.VMEM((M, rows, padded), f32),
                pltpu.VMEM((rows, padded), f32),
                pltpu.VMEM((CHUNKS, M, rows, chunk), f32),
                pltpu.VMEM((3, rows, LANE), f32),
                pltpu.VMEM((slices, 8, LANE), f32),
                pltpu.VMEM((M, 8, LANE), f32),
                dma((2, 3)),
                dma((CHUNKS,)), dma((CHUNKS,)), dma((CHUNKS,)),
                dma((CHUNKS,)), dma((CHUNKS,)), dma((CHUNKS,)),
                dma((CHUNKS, M)), dma((CHUNKS, M)), dma((CHUNKS,)),
                dma((slices,)), dma((slices,)), dma((M,)), dma((M,)),
            ],
            compiler_params=pltpu.CompilerParams(
                collective_id=0, has_side_effects=True, vmem_limit_bytes=48 * 1024 * 1024
            ),
        )(
            pltpu.with_memory_space_constraint(slice_starts, pltpu.HBM),
            pltpu.with_memory_space_constraint(coupling, pltpu.HBM),
        )
        return values, logs

    return jax.shard_map(
        body,
        mesh=mesh,
        in_specs=(P("tm", None, None), P()),
        out_specs=(P("tm", "node", None, None), P()),
        check_vma=False,
    )
```

```python
import functools
import jax
import jax.numpy as jnp
from jax import lax
from jax.experimental import pallas as pl
from jax.experimental.pallas import tpu as pltpu
from jax.sharding import PartitionSpec as P

M = 4
STEP = 8
FIRST = (4, 8, 12)
SLANT = 1
REST = 16
LANE = 128
HALO = 3
PAD = 4
PIECES = 4
MESH = pl.DeviceIdType.MESH

time_step = 0.5
log_floor = 0.05


def legendre_gap(point, node_count):
    before = 1.0
    current = point
    for degree in range(1, node_count):
        following = ((2 * degree + 1) * point * current - degree * before) / (degree + 1)
        before = current
        current = following
    return current - before


def collocation(node_count):
    points = []
    samples = 4000
    for sample_index in range(samples - 1):
        lower_end = -1.0 + 2.0 * sample_index / samples
        upper_end = -1.0 + 2.0 * (sample_index + 1) / samples
        lower_value = legendre_gap(lower_end, node_count)
        upper_value = legendre_gap(upper_end, node_count)
        if lower_value * upper_value < 0.0:
            for halving in range(80):
                middle = 0.5 * (lower_end + upper_end)
                middle_value = legendre_gap(middle, node_count)
                if lower_value * middle_value <= 0.0:
                    upper_end = middle
                else:
                    lower_end = middle
                    lower_value = middle_value
            points.append(0.5 * (lower_end + upper_end))
    points.append(1.0)
    node_times = [(point + 1.0) / 2.0 for point in points]
    matrix = [[0.0] * node_count for row_index in range(node_count)]
    for column in range(node_count):
        coeffs = [1.0]
        for other in range(node_count):
            if other != column:
                scale = node_times[column] - node_times[other]
                shifted = [0.0] + coeffs
                scaled = [value * node_times[other] for value in coeffs] + [0.0]
                coeffs = [(shifted[power] - scaled[power]) / scale for power in range(len(shifted))]
        for row_index in range(node_count):
            upper_time = node_times[row_index]
            matrix[row_index][column] = sum(
                (
                    coeffs[power] * upper_time ** (power + 1) / (power + 1)
                    for power in range(len(coeffs))
                )
            )
    return (node_times, matrix)


def plan(tiles):
    bounds = [0]
    for size in FIRST:
        bounds.append(bounds[-1] + size)
    while bounds[-1] < tiles:
        bounds.append(min(bounds[-1] + REST, tiles))
    return bounds


def kernel(
    slices, rows, cells,
    start_hbm, coupling_hbm, out_hbm, log_ref,
    log_tile, log_sem,
    own, couple, prev1, prev2, prev3, relay, here, there, mid, before, result,
    acc, part_tm, part_node,
    load_sem, s_prev1, r_prev1, s_prev2, r_prev2, s_prev3, r_prev3,
    s_relay, r_relay, s_side, s_diag, far,
    s_out, r_out, local_sem, s_tm, r_tm, s_node, r_node,
):
    p = lax.axis_index("tm")
    n = lax.axis_index("node")
    all_tiles = cells // LANE
    bounds = plan(all_tiles)
    chunks = len(bounds) - 1
    my_rows = pl.ds(pl.multiple_of(n * rows, rows), rows)
    node_times, matrix = collocation(M)
    weight = [[time_step * value for value in line] for line in matrix]
    total = [sum(line) for line in weight]
    implicit = [time_step * moment / M for moment in node_times]
    even = lax.rem(p, 2) == 0
    first = p == 0
    second = p == 1

    loads = []
    for index, (source, target) in enumerate(
        ((start_hbm.at[0, my_rows], own), (coupling_hbm.at[my_rows], couple))
    ):
        for piece, (lo, to, size) in enumerate(
            ((0, PAD * LANE, cells), (cells - HALO * LANE, LANE, HALO * LANE), (0, PAD * LANE + cells, HALO * LANE))
        ):
            copy = pltpu.make_async_copy(
                source.at[:, pl.ds(lo, size)],
                target.at[:, pl.ds(to, size)],
                load_sem.at[index],
            )
            copy.start()
        whole = cells + 2 * HALO * LANE
        loads.append(
            pltpu.make_async_copy(
                target.at[:, pl.ds(0, whole)], target.at[:, pl.ds(0, whole)], load_sem.at[index]
            )
        )

    partner = jnp.where(even, p + 1, p - 1)
    ahead = lax.rem(p + 2, slices)
    behind = lax.rem(p + slices - 2, slices)
    has_behind = p >= 2
    has_ahead = p + 2 < slices
    odd = jnp.logical_not(even)
    along = has_behind.astype(jnp.int32) + has_ahead.astype(jnp.int32)
    slanted = jnp.where(even, has_behind, has_ahead)
    slant = jnp.where(even, lax.rem(p + slices - 1, slices), lax.rem(p + 1, slices))

    def signal(semaphore, tm, node):
        pl.semaphore_signal(
            semaphore, inc=1, device_id={"tm": tm, "node": node}, device_id_type=MESH
        )

    def signal_along(semaphore):
        @pl.when(has_behind)
        def _():
            signal(semaphore, behind, n)

        @pl.when(has_ahead)
        def _():
            signal(semaphore, ahead, n)

    barrier = pltpu.get_barrier_semaphore()
    signal_along(barrier)

    @pl.when(slanted)
    def _():
        signal(barrier, slant, n)

    signal(barrier, partner, n)
    for step in range(1, M):
        signal(barrier, p, lax.rem(n + step, M))
    pl.semaphore_wait(barrier, along + slanted.astype(jnp.int32) + M)
    rounds = max(slices // 2 - 2, 0)

    def meet(index):
        if 0 < index <= rounds:
            pl.semaphore_wait(far.at[index - 1], along)
        if index < rounds:
            signal_along(far.at[index])
        if index == rounds:
            signal(far.at[rounds], partner, n)
        if index == rounds + 1:
            pl.semaphore_wait(far.at[rounds], 1)

    meet(0)
    for copy in loads:
        copy.wait()

    def shape_of(count):
        return prev3.at[:, pl.ds(0, count * LANE)]

    def remote(source, target, send, recv, tm, node):
        return pltpu.make_async_remote_copy(
            src_ref=source, dst_ref=target, send_sem=send, recv_sem=recv,
            device_id={"tm": tm, "node": node}, device_id_type=MESH,
        )

    def part(ref, c):
        begin = (bounds[c] + HALO if c else -HALO) + PAD
        end = bounds[c + 1] + HALO + PAD
        return ref.at[:, pl.ds(begin * LANE, (end - begin) * LANE)]

    def to_partner_own(c):
        return remote(part(own, c), part(prev1, c), s_prev1, r_prev1.at[c], partner, n)

    def to_partner_forward(c):
        return remote(part(prev2, c), part(prev1, c), s_prev1, r_prev1.at[c], partner, n)

    def slant_own(c):
        return remote(part(own, c), part(prev1, c), s_diag, r_prev1.at[c], slant, n)

    def ahead_own(c):
        return remote(part(own, c), part(prev2, c), s_prev2, r_prev2.at[c], ahead, n)

    def ahead_forward(c):
        return remote(part(prev1, c), part(prev3, c), s_prev3, r_prev3.at[c], ahead, n)

    def relay_forward(c):
        return remote(part(prev2, c), part(relay, c), s_relay, r_relay.at[c], ahead, n)

    def to_partner_relayed(c):
        return remote(part(relay, c), part(prev3, c), s_side, r_prev3.at[c], partner, n)

    def to_partner_second(c):
        return remote(part(prev2, c), part(prev3, c), s_side, r_prev3.at[c], partner, n)

    def relayed(c):
        return c % 3 == 2

    def crossed(c):
        return c % 3 != 1

    def sends_third(c):
        if relayed(c):
            return None
        if crossed(c):
            return jnp.logical_and(has_ahead, jnp.logical_and(even, has_behind))
        return jnp.logical_and(has_ahead, jnp.logical_not(first))

    def start_ahead(c):
        @pl.when(has_ahead)
        def _():
            ahead_own(c).start()

        @pl.when(even)
        def _():
            to_partner_own(c).start()

    def pass_across(c):
        @pl.when(has_behind)
        def _():
            ahead_own(c).wait_recv()

        @pl.when(jnp.logical_and(odd, has_behind))
        def _():
            if c >= SLANT:
                to_partner_forward(c).start()
            if relayed(c):

                @pl.when(has_ahead)
                def _():
                    relay_forward(c).start()

        if crossed(c):

            @pl.when(jnp.logical_and(even, has_behind))
            def _():
                to_partner_second(c).start()

    def pass_back(c):
        if relayed(c):

            @pl.when(jnp.logical_and(odd, p >= 5))
            def _():
                relay_forward(c).wait_recv()
                to_partner_relayed(c).start()

    def pass_ahead(c):
        @pl.when(odd)
        def _():
            to_partner_own(c).wait_recv()

        @pl.when(jnp.logical_and(even, has_behind))
        def _():
            to_partner_forward(c).wait_recv()

        if not relayed(c):

            @pl.when(sends_third(c))
            def _():
                ahead_forward(c).start()

    for c in range(SLANT):

        @pl.when(jnp.logical_and(odd, has_ahead))
        def _():
            slant_own(c).start()

    for c in range(min(3, chunks)):
        start_ahead(c)

    acc[...] = jnp.zeros_like(acc)

    def diffusion(v, c, k):
        size = (k + 2) * LANE
        right = pltpu.roll(v, size - 1, 1)
        flux = c * (right - v)
        left = pltpu.roll(flux, 1, 1)
        return (flux - left)[:, LANE:LANE + k * LANE]

    def two_steps(base, u, square, reaction, a):
        s = (3.0 * a) * square - a
        d = 1.0 + s
        top = base + u * s
        target = base - a * reaction
        dd = d * d
        tt = top * top
        above = target * (d * dd) + (2.0 * a) * (top * tt)
        below = d * ((1.0 - a) * dd + (3.0 * a) * tt)
        guess = pl.reciprocal(below, approx=True)
        return above * (guess * (2.0 - below * guess))

    def folded(value, k):
        out = value[:, :LANE]
        for piece in range(1, k):
            out = out + value[:, piece * LANE:(piece + 1) * LANE]
        return out

    def run(begin, end, block, counted):
        count = (end - begin) // STEP

        def step(i, carry):
            block(begin + i * STEP, STEP, counted)
            return carry

        lax.fori_loop(0, count, step, 0)
        if begin + count * STEP < end:
            block(begin + count * STEP, end - begin - count * STEP, counted)

    def over(c, lag, block):
        begin = bounds[c] + lag if c else 0
        end = min(bounds[c + 1] + lag, all_tiles)
        if c == 0 and lag:
            block(-lag, lag, False)
        run(begin, end, block, True)
        if c == chunks - 1 and lag:
            block(all_tiles, lag, False)

    def lanes(offset):
        return offset * LANE if isinstance(offset, int) else pl.multiple_of(offset * LANE, LANE)

    def wide(tile, k):
        return pl.ds(lanes(tile + PAD - 1), (k + 2) * LANE)

    def centre(tile, k):
        return pl.ds(lanes(tile + PAD), k * LANE)

    pass_across(0)
    pass_ahead(0)
    start_ahead(3)
    pass_across(1)
    pass_ahead(1)
    start_ahead(4)
    pass_across(2)
    start_ahead(5)
    pass_across(3)
    for c in range(chunks):
        base_lane = bounds[c] * LANE
        chunk = (bounds[c + 1] - bounds[c]) * LANE

        if c + 6 < chunks:
            start_ahead(c + 6)
        if c + 2 < chunks:
            pass_ahead(c + 2)

        @pl.when(p >= 3)
        def _():
            ahead_forward(c).wait_recv()

        def stage_a(tile, k, counted):
            mid_slice = slice(LANE, LANE + k * LANE)
            cw = couple[:, wide(tile, k)]
            at = centre(tile, k)
            vw = own[:, wide(tile, k)]
            v = vw[:, mid_slice]
            p1w = jnp.where(first, vw, prev1[:, wide(tile, k)])
            p1 = p1w[:, mid_slice]
            p2w = jnp.where(p <= 1, p1w, prev2[:, wide(tile, k)])
            p2 = p2w[:, mid_slice]
            p3 = jnp.where(p <= 2, p2, prev3[:, at])

            square = v * v
            reaction = v - v * square
            forcing = diffusion(vw, cw, k) + reaction
            found = None
            for m in range(M):
                base = p1 + total[m] * forcing
                if counted:
                    defect = base - v
                    found = defect * defect if found is None else found + defect * defect
                here[m, :, at] = two_steps(base, v, square, reaction, implicit[m])
            if counted:
                acc[0] += folded(found, k)

            square = p1 * p1
            reaction = p1 - p1 * square
            forcing = diffusion(p1w, cw, k) + reaction
            for m in range(M):
                there[m, :, at] = two_steps(p2 + total[m] * forcing, p1, square, reaction, implicit[m])

            square = p2 * p2
            reaction = p2 - p2 * square
            forcing = diffusion(p2w, cw, k) + reaction
            last = two_steps(
                p3 + total[M - 1] * forcing, p2, square, reaction, implicit[M - 1]
            )
            before[:, at] = jnp.where(second, p1, last)

        over(c, 2, stage_a)
        if c + 4 < chunks:
            pass_across(c + 4)
        if c + 2 < chunks:
            pass_back(c + 2)

        def update(source, begin, cw, tile, k, which, counted):
            values = []
            forcings = []
            for m in range(M):
                vw = source[m, :, wide(tile, k)]
                v = vw[:, LANE:LANE + k * LANE]
                square = v * v
                reaction = v - v * square
                values.append((v, square, reaction))
                forcings.append(diffusion(vw, cw, k) + reaction)
            found = None
            outputs = []
            for m in range(M):
                base = begin
                for j in range(M):
                    base = base + weight[m][j] * forcings[j]
                v, square, reaction = values[m]
                if counted:
                    defect = base - v
                    found = defect * defect if found is None else found + defect * defect
                outputs.append(two_steps(base, v, square, reaction, implicit[m]))
            if counted:
                acc[which] += folded(found, k)
            return outputs

        def stage_b(tile, k, counted):
            cw = couple[:, wide(tile, k)]
            at = centre(tile, k)
            begin = jnp.where(first, own[:, centre(tile, k)], there[M - 1, :, at])
            outputs = update(here, begin, cw, tile, k, 1, counted)
            for m in range(M):
                mid[m, :, at] = outputs[m]
            mixed = None
            mixed_reaction = None
            for m in range(M):
                w = weight[M - 1][m]
                vw = there[m, :, wide(tile, k)]
                v = vw[:, LANE:LANE + k * LANE]
                square = v * v
                reaction = v - v * square
                mixed = w * vw if mixed is None else mixed + w * vw
                mixed_reaction = w * reaction if mixed_reaction is None else mixed_reaction + w * reaction
            base = before[:, at] + (diffusion(mixed, cw, k) + mixed_reaction)
            last = two_steps(base, v, square, reaction, implicit[M - 1])
            before[:, at] = jnp.where(first, own[:, centre(tile, k)], last)

        over(c, 1, stage_b)

        def stage_c(tile, k, counted):
            cw = couple[:, wide(tile, k)]
            outputs = update(mid, before[:, centre(tile, k)], cw, tile, k, 2, counted)
            at = pl.ds(lanes(tile), k * LANE)
            for m in range(M):
                result[m, :, at] = outputs[m]

        over(c, 0, stage_c)

        if c >= 2:
            meet(c - 1)
        here_cells = pl.ds(base_lane, chunk)
        target = out_hbm.at[0, 0, my_rows, here_cells]
        for step in (2, 3, 1):
            peer = lax.rem(n + step, M)
            remote(result.at[peer, :, here_cells], target, s_out, r_out, p, peer).start()
        pltpu.make_async_copy(result.at[n, :, here_cells], target, local_sem).start()

    for index in range(max(chunks - 1, 1), rounds + 2):
        meet(index)
    lane = lax.broadcasted_iota(jnp.int32, (rows, LANE), 1)
    sub = lax.broadcasted_iota(jnp.int32, (rows, LANE), 0)
    place = lax.broadcasted_iota(jnp.int32, (8, LANE), 0)
    tile_value = jnp.zeros((8, LANE), jnp.float32)
    for which in range(3):
        per_system = jnp.sum(acc[which], axis=1, keepdims=True)
        row = jnp.sum(
            jnp.where(lane == n * rows + sub, per_system, 0.0), axis=0, keepdims=True
        )
        tile_value = tile_value + jnp.where(place == which, row, 0.0)
    part_tm[p] = tile_value
    for step in range(1, slices):
        copy = remote(
            part_tm.at[p], part_tm.at[p], s_tm, r_tm, lax.rem(p + step, slices), n
        )
        copy.start()
    others = part_tm.at[pl.ds(0, slices - 1)]
    gathered = remote(others, others, s_tm, r_tm, partner, n)
    gathered.wait_recv()
    summed = part_tm[0]
    for index in range(1, slices):
        summed = summed + part_tm[index]
    part_node[n] = summed
    for step in range(1, M):
        copy = remote(
            part_node.at[n], part_node.at[n], s_node, r_node, p, lax.rem(n + step, M)
        )
        copy.start()
    others = part_node.at[pl.ds(0, M - 1)]
    spread = remote(others, others, s_node, r_node, partner, n)
    spread.wait_recv()
    summed = part_node[0]
    for index in range(1, M):
        summed = summed + part_node[index]
    log_tile[...] = jnp.log(log_floor + summed / (slices * M * cells))[:3, :M * rows]
    log_copy = pltpu.make_async_copy(log_tile, log_ref, log_sem)
    log_copy.start()

    log_copy.wait()
    gathered.wait_send()
    spread.wait_send()
    three = result.at[pl.ds(0, M - 1)]
    outputs = remote(three, three, s_out, r_out, partner, n)
    outputs.wait_send()
    outputs.wait_recv()
    mine = result.at[0]
    pltpu.make_async_copy(mine, mine, local_sem).wait()

    def span(c):
        return bounds[c + 1] - bounds[c] + (0 if c else 2 * HALO)

    def drain(semaphore, wanted):
        count = sum(span(c) for c in range(chunks) if wanted(c))
        if count:
            remote(shape_of(count), shape_of(count), semaphore, r_prev3.at[0], partner, n).wait_send()

    def direct(c):
        return not relayed(c)

    def straight(c):
        return not crossed(c)

    @pl.when(has_ahead)
    def _():
        drain(s_prev2, lambda c: True)

    @pl.when(jnp.logical_and(has_ahead, jnp.logical_and(even, has_behind)))
    def _():
        drain(s_prev3, direct)

    @pl.when(jnp.logical_and(has_ahead, odd))
    def _():
        drain(s_prev3, straight)
        drain(s_diag, lambda c: c < SLANT)

    @pl.when(even)
    def _():
        drain(s_prev1, lambda c: True)

    @pl.when(jnp.logical_and(odd, has_behind))
    def _():
        drain(s_prev1, lambda c: c >= SLANT)

    @pl.when(jnp.logical_and(has_ahead, jnp.logical_and(odd, has_behind)))
    def _():
        drain(s_relay, relayed)

    @pl.when(jnp.logical_and(odd, p >= 5))
    def _():
        drain(s_side, relayed)

    @pl.when(jnp.logical_and(even, has_behind))
    def _():
        drain(s_side, crossed)


def unload(values, logs, values_hbm, logs_hbm, sem):
    size = values.shape[2] // PIECES
    copies = [pltpu.make_async_copy(logs, logs_hbm, sem.at[PIECES])]
    for piece in range(PIECES):
        at = pl.ds(piece * size, size)
        copies.append(
            pltpu.make_async_copy(values.at[:, :, at], values_hbm.at[:, :, at], sem.at[piece])
        )
    for copy in copies:
        copy.start()
    for copy in copies:
        copy.wait()


def solution(mesh):
    slices = mesh.shape["tm"]

    def body(slice_starts, coupling):
        systems, cells = coupling.shape
        rows = systems // M
        chunks = len(plan(cells // LANE)) - 1
        far = max(slices // 2 - 2, 0) + 1
        padded = cells + 2 * PAD * LANE
        f32 = jnp.float32
        dma = pltpu.SemaphoreType.DMA
        anyplace = pl.BlockSpec(memory_space=pl.ANY)
        anywhere = pl.BlockSpec(memory_space=pltpu.HBM)
        values, logs = pl.pallas_call(
            functools.partial(kernel, slices, rows, cells),
            out_shape=(
                jax.ShapeDtypeStruct((1, 1, systems, cells), f32),
                jax.ShapeDtypeStruct((3, systems), f32),
            ),
            in_specs=[anywhere, anywhere],
            out_specs=(anyplace, anyplace),
            scratch_shapes=[
                pltpu.VMEM((3, systems), f32), dma,
                pltpu.VMEM((rows, padded), f32),
                pltpu.VMEM((rows, padded), f32),
                pltpu.VMEM((rows, padded), f32),
                pltpu.VMEM((rows, padded), f32),
                pltpu.VMEM((rows, padded), f32),
                pltpu.VMEM((rows, padded), f32),
                pltpu.VMEM((M, rows, padded), f32),
                pltpu.VMEM((M, rows, padded), f32),
                pltpu.VMEM((M, rows, padded), f32),
                pltpu.VMEM((rows, padded), f32),
                pltpu.VMEM((M, rows, cells), f32),
                pltpu.VMEM((3, rows, LANE), f32),
                pltpu.VMEM((slices, 8, LANE), f32),
                pltpu.VMEM((M, 8, LANE), f32),
                dma((2,)),
                dma, dma((chunks,)), dma, dma((chunks,)), dma, dma((chunks,)),
                dma, dma((chunks,)), dma, dma, pltpu.SemaphoreType.REGULAR((far,)),
                dma, dma, dma, dma, dma, dma, dma,
            ],
            compiler_params=pltpu.CompilerParams(
                collective_id=0, has_side_effects=True, vmem_limit_bytes=48 * 1024 * 1024
            ),
        )(
            pltpu.with_memory_space_constraint(slice_starts, pltpu.HBM),
            pltpu.with_memory_space_constraint(coupling, pltpu.HBM),
        )
        return tuple(
            pl.pallas_call(
                unload,
                out_shape=(pltpu.HBM(values.shape, f32), pltpu.HBM(logs.shape, f32)),
                in_specs=[anyplace, anyplace],
                out_specs=(anywhere, anywhere),
                scratch_shapes=[dma((PIECES + 1,))],
                compiler_params=pltpu.CompilerParams(vmem_limit_bytes=1024 * 1024),
            )(values, logs)
        )

    return jax.shard_map(
        body,
        mesh=mesh,
        in_specs=(P("tm", None, None), P()),
        out_specs=(P("tm", "node", None, None), P()),
        check_vma=False,
    )
```

```python
import functools
import jax
import jax.numpy as jnp
from jax import lax
from jax.experimental import pallas as pl
from jax.experimental.pallas import tpu as pltpu
from jax.sharding import PartitionSpec as P

M = 4
STEP = 16
FIRST = (4, 8, 12)
SLANT = 2
KINDS = (1, 1, 1, 2, 0, 1, 2, 0, 1, 2, 0)
START = (("even", 3), ("odd", 4), ("across", 1), ("ahead", 1), ("even", 4), ("across", 2), ("ahead", 2), ("even", 5), ("odd", 5), ("across", 3))
STEADY = ((0, "odd", 6), (1, "ahead", 3), (1, "even", 6), (2, "across", 5), (2, "back", 3))
EARLY = {(0, "ahead"): 2, (1, "ahead"): 2, (0, "across"): 4, (1, "across"): 4, (0, "back"): 1, (1, "back"): 2}
REST = 16
LANE = 128
HALO = 3
PAD = 4
PIECES = 1
MESH = pl.DeviceIdType.MESH

time_step = 0.5
log_floor = 0.05


def legendre_gap(point, node_count):
    before = 1.0
    current = point
    for degree in range(1, node_count):
        following = ((2 * degree + 1) * point * current - degree * before) / (degree + 1)
        before = current
        current = following
    return current - before


def collocation(node_count):
    points = []
    samples = 4000
    for sample_index in range(samples - 1):
        lower_end = -1.0 + 2.0 * sample_index / samples
        upper_end = -1.0 + 2.0 * (sample_index + 1) / samples
        lower_value = legendre_gap(lower_end, node_count)
        upper_value = legendre_gap(upper_end, node_count)
        if lower_value * upper_value < 0.0:
            for halving in range(80):
                middle = 0.5 * (lower_end + upper_end)
                middle_value = legendre_gap(middle, node_count)
                if lower_value * middle_value <= 0.0:
                    upper_end = middle
                else:
                    lower_end = middle
                    lower_value = middle_value
            points.append(0.5 * (lower_end + upper_end))
    points.append(1.0)
    node_times = [(point + 1.0) / 2.0 for point in points]
    matrix = [[0.0] * node_count for row_index in range(node_count)]
    for column in range(node_count):
        coeffs = [1.0]
        for other in range(node_count):
            if other != column:
                scale = node_times[column] - node_times[other]
                shifted = [0.0] + coeffs
                scaled = [value * node_times[other] for value in coeffs] + [0.0]
                coeffs = [(shifted[power] - scaled[power]) / scale for power in range(len(shifted))]
        for row_index in range(node_count):
            upper_time = node_times[row_index]
            matrix[row_index][column] = sum(
                (
                    coeffs[power] * upper_time ** (power + 1) / (power + 1)
                    for power in range(len(coeffs))
                )
            )
    return (node_times, matrix)


def plan(tiles):
    bounds = [0]
    for size in FIRST:
        bounds.append(bounds[-1] + size)
    while bounds[-1] < tiles:
        bounds.append(min(bounds[-1] + REST, tiles))
    return bounds


def kernel(
    slices, rows, cells,
    start_hbm, coupling_hbm, out_hbm, log_ref,
    log_tile, log_sem,
    own, couple, prev1, prev2, prev3, relay, here, there, mid, before, result,
    acc, part_tm, part_node,
    load_sem, s_prev1, r_prev1, s_prev2, r_prev2, s_prev3, r_prev3,
    s_relay, r_relay, s_side, s_diag, far,
    s_out, r_out, local_sem, s_tm, r_tm, s_node, r_node,
):
    p = lax.axis_index("tm")
    n = lax.axis_index("node")
    all_tiles = cells // LANE
    bounds = plan(all_tiles)
    chunks = len(bounds) - 1
    my_rows = pl.ds(pl.multiple_of(n * rows, rows), rows)
    node_times, matrix = collocation(M)
    weight = [[time_step * value for value in line] for line in matrix]
    implicit = [time_step * moment / M for moment in node_times]
    even = lax.rem(p, 2) == 0
    first = p == 0
    second = p == 1

    loads = []
    for index, (source, target) in enumerate(
        ((start_hbm.at[0, my_rows], own), (coupling_hbm.at[my_rows], couple))
    ):
        for piece, (lo, to, size) in enumerate(
            ((0, PAD * LANE, cells), (cells - HALO * LANE, LANE, HALO * LANE), (0, PAD * LANE + cells, HALO * LANE))
        ):
            copy = pltpu.make_async_copy(
                source.at[:, pl.ds(lo, size)],
                target.at[:, pl.ds(to, size)],
                load_sem.at[index],
            )
            copy.start()
        whole = cells + 2 * HALO * LANE
        loads.append(
            pltpu.make_async_copy(
                target.at[:, pl.ds(0, whole)], target.at[:, pl.ds(0, whole)], load_sem.at[index]
            )
        )

    partner = jnp.where(even, p + 1, p - 1)
    ahead = lax.rem(p + 2, slices)
    behind = lax.rem(p + slices - 2, slices)
    has_behind = p >= 2
    has_ahead = p + 2 < slices
    odd = jnp.logical_not(even)
    along = has_behind.astype(jnp.int32) + has_ahead.astype(jnp.int32)
    slanted = jnp.where(even, has_behind, has_ahead)
    slant = jnp.where(even, lax.rem(p + slices - 1, slices), lax.rem(p + 1, slices))

    def signal(semaphore, tm, node):
        pl.semaphore_signal(
            semaphore, inc=1, device_id={"tm": tm, "node": node}, device_id_type=MESH
        )

    def signal_along(semaphore):
        @pl.when(has_behind)
        def _():
            signal(semaphore, behind, n)

        @pl.when(has_ahead)
        def _():
            signal(semaphore, ahead, n)

    barrier = pltpu.get_barrier_semaphore()
    signal_along(barrier)

    @pl.when(slanted)
    def _():
        signal(barrier, slant, n)

    signal(barrier, partner, n)
    for step in range(1, M):
        signal(barrier, p, lax.rem(n + step, M))
    pl.semaphore_wait(barrier, along + slanted.astype(jnp.int32) + M)
    rounds = max(slices // 2 - 2, 0)

    def meet(index):
        if 0 < index <= rounds:
            pl.semaphore_wait(far.at[index - 1], along)
        if index < rounds:
            signal_along(far.at[index])
        if index == rounds:
            signal(far.at[rounds], partner, n)
        if index == rounds + 1:
            pl.semaphore_wait(far.at[rounds], 1)

    meet(0)
    for copy in loads:
        copy.wait()

    def shape_of(count):
        return prev3.at[:, pl.ds(0, count * LANE)]

    def remote(source, target, send, recv, tm, node):
        return pltpu.make_async_remote_copy(
            src_ref=source, dst_ref=target, send_sem=send, recv_sem=recv,
            device_id={"tm": tm, "node": node}, device_id_type=MESH,
        )

    def part(ref, c):
        begin = (bounds[c] + HALO if c else -HALO) + PAD
        end = bounds[c + 1] + HALO + PAD
        return ref.at[:, pl.ds(begin * LANE, (end - begin) * LANE)]

    def to_partner_own(c):
        return remote(part(own, c), part(prev1, c), s_prev1, r_prev1.at[c], partner, n)

    def to_partner_forward(c):
        return remote(part(prev2, c), part(prev1, c), s_prev1, r_prev1.at[c], partner, n)

    def slant_own(c):
        return remote(part(own, c), part(prev1, c), s_diag, r_prev1.at[c], slant, n)

    def ahead_own(c):
        return remote(part(own, c), part(prev2, c), s_prev2, r_prev2.at[c], ahead, n)

    def ahead_forward(c):
        return remote(part(prev1, c), part(prev3, c), s_prev3, r_prev3.at[c], ahead, n)

    def relay_forward(c):
        return remote(part(prev2, c), part(relay, c), s_relay, r_relay.at[c], ahead, n)

    def to_partner_relayed(c):
        return remote(part(relay, c), part(prev3, c), s_side, r_prev3.at[c], partner, n)

    def to_partner_second(c):
        return remote(part(prev2, c), part(prev3, c), s_side, r_prev3.at[c], partner, n)

    def relayed(c):
        return KINDS[c % len(KINDS)] == 0

    def crossed(c):
        return KINDS[c % len(KINDS)] != 2

    def sends_third(c):
        if relayed(c):
            return None
        if crossed(c):
            return jnp.logical_and(has_ahead, jnp.logical_and(even, has_behind))
        return jnp.logical_and(has_ahead, jnp.logical_not(first))

    def start_even(c):
        @pl.when(even)
        def _():
            to_partner_own(c).start()

            @pl.when(has_ahead)
            def _():
                ahead_own(c).start()

    def start_odd(c):
        @pl.when(jnp.logical_and(odd, has_ahead))
        def _():
            if c < SLANT:
                slant_own(c).start()
            ahead_own(c).start()

    def pass_across(c):
        @pl.when(has_behind)
        def _():
            ahead_own(c).wait_recv()

        @pl.when(jnp.logical_and(odd, has_behind))
        def _():
            if c >= SLANT:
                to_partner_forward(c).start()
            if relayed(c):

                @pl.when(has_ahead)
                def _():
                    relay_forward(c).start()

        if crossed(c):

            @pl.when(jnp.logical_and(even, has_behind))
            def _():
                to_partner_second(c).start()

    def pass_back(c):
        if relayed(c):

            @pl.when(jnp.logical_and(odd, p >= 5))
            def _():
                relay_forward(c).wait_recv()
                to_partner_relayed(c).start()

    def pass_ahead(c):
        @pl.when(odd)
        def _():
            to_partner_own(c).wait_recv()

        @pl.when(jnp.logical_and(even, has_behind))
        def _():
            to_partner_forward(c).wait_recv()

        if not relayed(c):

            @pl.when(sends_third(c))
            def _():
                ahead_forward(c).start()

    acc[...] = jnp.zeros_like(acc)

    def diffusion(v, c, k):
        size = (k + 2) * LANE
        right = pltpu.roll(v, size - 1, 1)
        flux = c * (right - v)
        left = pltpu.roll(flux, 1, 1)
        return (flux - left)[:, LANE:LANE + k * LANE]

    def finish(d, top, target, a):
        dd = d * d
        tt = top * top
        above = target * (d * dd) + (2.0 * a) * (top * tt)
        below = d * ((1.0 - a) * dd + (3.0 * a) * tt)
        guess = pl.reciprocal(below, approx=True)
        return above * (guess * (2.0 - below * guess))

    def two_steps(base, defect, u, square, reaction, a):
        d = (3.0 * a) * square + (1.0 - a)
        return finish(d, defect + u * d, base - a * reaction, a)

    def equal_nodes(begin, vw, cw, k):
        v = vw[:, LANE:LANE + k * LANE]
        square = v * v
        reaction = v - v * square
        four = 4.0 * (diffusion(vw, cw, k) + reaction)
        slope = 3.0 * square - 1.0
        lift = four + v * slope
        pull = four - reaction

        def node(m):
            a = implicit[m]
            return finish(1.0 + a * slope, begin + a * lift, begin + a * pull, a)

        return v, four, node

    def folded(value, k):
        out = value[:, :LANE]
        for piece in range(1, k):
            out = out + value[:, piece * LANE:(piece + 1) * LANE]
        return out

    def run(begin, end, block, counted):
        count = (end - begin) // STEP

        def step(i, carry):
            block(begin + i * STEP, STEP, counted)
            return carry

        lax.fori_loop(0, count, step, 0)
        if begin + count * STEP < end:
            block(begin + count * STEP, end - begin - count * STEP, counted)

    def over(c, lag, block):
        begin = bounds[c] + lag if c else 0
        end = min(bounds[c + 1] + lag, all_tiles)
        if c == 0 and lag:
            block(-lag, lag, False)
        run(begin, end, block, True)
        if c == chunks - 1 and lag:
            block(all_tiles, lag, False)

    def lanes(offset):
        return offset * LANE if isinstance(offset, int) else pl.multiple_of(offset * LANE, LANE)

    def wide(tile, k):
        return pl.ds(lanes(tile + PAD - 1), (k + 2) * LANE)

    def centre(tile, k):
        return pl.ds(lanes(tile + PAD), k * LANE)

    begun = {"even": 0, "odd": 0, "across": 0, "ahead": 0, "back": 0}
    moves = {
        "even": start_even, "odd": start_odd,
        "across": pass_across, "ahead": pass_ahead, "back": pass_back,
    }

    def proceed(name, upto):
        for index in range(begun[name], min(upto, chunks)):
            moves[name](index)
        begun[name] = max(begun[name], upto)

    for name, upto in START:
        proceed(name, upto)

    def stage(k, place):
        for at, name, lead in STEADY:
            if at == place:
                slack = EARLY.get((k, name), lead)
                proceed(name, k + slack)

    for c in range(chunks):
        base_lane = bounds[c] * LANE
        chunk = (bounds[c + 1] - bounds[c]) * LANE

        stage(c, 0)
        for name in moves:
            proceed(name, c + 1)

        @pl.when(p >= 3)
        def _():
            ahead_forward(c).wait_recv()

        def stage_a(tile, k, counted):
            middle = slice(LANE, LANE + k * LANE)
            cw = couple[:, wide(tile, k)]
            at = centre(tile, k)
            vw = own[:, wide(tile, k)]
            p1w = jnp.where(first, vw, prev1[:, wide(tile, k)])
            p1 = p1w[:, middle]
            p2w = jnp.where(p <= 1, p1w, prev2[:, wide(tile, k)])
            p2 = p2w[:, middle]
            p3 = jnp.where(p <= 2, p2, prev3[:, at])

            v, four, node = equal_nodes(p1, vw, cw, k)
            for m in range(M):
                here[m, :, at] = node(m)
            if counted:
                gap = p1 - v
                cross = 2.0 * sum(implicit)
                curve = sum(a * a for a in implicit)
                acc[0] += folded(
                    gap * (float(M) * gap + cross * four) + curve * (four * four), k
                )

            _, _, node = equal_nodes(p2, p1w, cw, k)
            for m in range(M):
                there[m, :, at] = node(m)

            _, _, node = equal_nodes(p3, p2w, cw, k)
            before[:, at] = jnp.where(second, p1, node(M - 1))

        over(c, 2, stage_a)
        stage(c, 1)

        def update(source, begin, cw, tile, k, which, counted):
            values = []
            forcings = []
            for m in range(M):
                vw = source[m, :, wide(tile, k)]
                v = vw[:, LANE:LANE + k * LANE]
                square = v * v
                reaction = v - v * square
                values.append((v, square, reaction))
                forcings.append(diffusion(vw, cw, k) + reaction)
            found = None
            outputs = []
            for m in range(M):
                base = begin
                for j in range(M):
                    base = base + weight[m][j] * forcings[j]
                v, square, reaction = values[m]
                defect = base - v
                if counted:
                    found = defect * defect if found is None else found + defect * defect
                outputs.append(two_steps(base, defect, v, square, reaction, implicit[m]))
            if counted:
                acc[which] += folded(found, k)
            return outputs

        def stage_b(tile, k, counted):
            cw = couple[:, wide(tile, k)]
            at = centre(tile, k)
            begin = jnp.where(first, own[:, centre(tile, k)], there[M - 1, :, at])
            outputs = update(here, begin, cw, tile, k, 1, counted)
            for m in range(M):
                mid[m, :, at] = outputs[m]
            mixed = None
            mixed_reaction = None
            for m in range(M):
                w = weight[M - 1][m]
                vw = there[m, :, wide(tile, k)]
                v = vw[:, LANE:LANE + k * LANE]
                square = v * v
                reaction = v - v * square
                mixed = w * vw if mixed is None else mixed + w * vw
                mixed_reaction = w * reaction if mixed_reaction is None else mixed_reaction + w * reaction
            base = before[:, at] + (diffusion(mixed, cw, k) + mixed_reaction)
            last = two_steps(base, base - v, v, square, reaction, implicit[M - 1])
            before[:, at] = jnp.where(first, own[:, centre(tile, k)], last)

        over(c, 1, stage_b)
        stage(c, 2)

        def stage_c(tile, k, counted):
            cw = couple[:, wide(tile, k)]
            outputs = update(mid, before[:, centre(tile, k)], cw, tile, k, 2, counted)
            at = pl.ds(lanes(tile), k * LANE)
            for m in range(M):
                result[m, :, at] = outputs[m]

        over(c, 0, stage_c)

        if c >= 2:
            meet(c - 1)
        here_cells = pl.ds(base_lane, chunk)
        target = out_hbm.at[0, 0, my_rows, here_cells]
        for step in (2, 3, 1):
            peer = lax.rem(n + step, M)
            remote(result.at[peer, :, here_cells], target, s_out, r_out, p, peer).start()
        pltpu.make_async_copy(result.at[n, :, here_cells], target, local_sem).start()

    for index in range(max(chunks - 1, 1), rounds + 2):
        meet(index)
    lane = lax.broadcasted_iota(jnp.int32, (rows, LANE), 1)
    sub = lax.broadcasted_iota(jnp.int32, (rows, LANE), 0)
    place = lax.broadcasted_iota(jnp.int32, (8, LANE), 0)
    tile_value = jnp.zeros((8, LANE), jnp.float32)
    for which in range(3):
        per_system = jnp.sum(acc[which], axis=1, keepdims=True)
        row = jnp.sum(
            jnp.where(lane == n * rows + sub, per_system, 0.0), axis=0, keepdims=True
        )
        tile_value = tile_value + jnp.where(place == which, row, 0.0)
    part_tm[p] = tile_value
    for step in range(1, slices):
        copy = remote(
            part_tm.at[p], part_tm.at[p], s_tm, r_tm, lax.rem(p + step, slices), n
        )
        copy.start()
    others = part_tm.at[pl.ds(0, slices - 1)]
    gathered = remote(others, others, s_tm, r_tm, partner, n)
    gathered.wait_recv()
    summed = part_tm[0]
    for index in range(1, slices):
        summed = summed + part_tm[index]
    part_node[n] = summed
    for step in range(1, M):
        copy = remote(
            part_node.at[n], part_node.at[n], s_node, r_node, p, lax.rem(n + step, M)
        )
        copy.start()
    others = part_node.at[pl.ds(0, M - 1)]
    spread = remote(others, others, s_node, r_node, partner, n)
    spread.wait_recv()
    summed = part_node[0]
    for index in range(1, M):
        summed = summed + part_node[index]
    log_tile[...] = jnp.log(log_floor + summed / (slices * M * cells))[:3, :M * rows]
    log_copy = pltpu.make_async_copy(log_tile, log_ref, log_sem)
    log_copy.start()

    log_copy.wait()
    gathered.wait_send()
    spread.wait_send()
    three = result.at[pl.ds(0, M - 1)]
    outputs = remote(three, three, s_out, r_out, partner, n)
    outputs.wait_send()
    outputs.wait_recv()
    mine = result.at[0]
    pltpu.make_async_copy(mine, mine, local_sem).wait()

    def span(c):
        return bounds[c + 1] - bounds[c] + (0 if c else 2 * HALO)

    def drain(semaphore, wanted):
        count = sum(span(c) for c in range(chunks) if wanted(c))
        if count:
            remote(shape_of(count), shape_of(count), semaphore, r_prev3.at[0], partner, n).wait_send()

    def direct(c):
        return not relayed(c)

    def straight(c):
        return not crossed(c)

    @pl.when(has_ahead)
    def _():
        drain(s_prev2, lambda c: True)

    @pl.when(jnp.logical_and(has_ahead, jnp.logical_and(even, has_behind)))
    def _():
        drain(s_prev3, direct)

    @pl.when(jnp.logical_and(has_ahead, odd))
    def _():
        drain(s_prev3, straight)
        drain(s_diag, lambda c: c < SLANT)

    @pl.when(even)
    def _():
        drain(s_prev1, lambda c: True)

    @pl.when(jnp.logical_and(odd, has_behind))
    def _():
        drain(s_prev1, lambda c: c >= SLANT)

    @pl.when(jnp.logical_and(has_ahead, jnp.logical_and(odd, has_behind)))
    def _():
        drain(s_relay, relayed)

    @pl.when(jnp.logical_and(odd, p >= 5))
    def _():
        drain(s_side, relayed)

    @pl.when(jnp.logical_and(even, has_behind))
    def _():
        drain(s_side, crossed)


def unload(values, logs, values_hbm, logs_hbm, sem):
    size = values.shape[2] // PIECES
    copies = [pltpu.make_async_copy(logs, logs_hbm, sem.at[PIECES])]
    for piece in range(PIECES):
        at = pl.ds(piece * size, size)
        copies.append(
            pltpu.make_async_copy(values.at[:, :, at], values_hbm.at[:, :, at], sem.at[piece])
        )
    for copy in copies:
        copy.start()
    for copy in copies:
        copy.wait()


def solution(mesh):
    slices = mesh.shape["tm"]

    def body(slice_starts, coupling):
        systems, cells = coupling.shape
        rows = systems // M
        chunks = len(plan(cells // LANE)) - 1
        far = max(slices // 2 - 2, 0) + 1
        padded = cells + 2 * PAD * LANE
        f32 = jnp.float32
        dma = pltpu.SemaphoreType.DMA
        anyplace = pl.BlockSpec(memory_space=pl.ANY)
        anywhere = pl.BlockSpec(memory_space=pltpu.HBM)
        values, logs = pl.pallas_call(
            functools.partial(kernel, slices, rows, cells),
            out_shape=(
                jax.ShapeDtypeStruct((1, 1, systems, cells), f32),
                jax.ShapeDtypeStruct((3, systems), f32),
            ),
            in_specs=[anywhere, anywhere],
            out_specs=(anyplace, anyplace),
            scratch_shapes=[
                pltpu.VMEM((3, systems), f32), dma,
                pltpu.VMEM((rows, padded), f32),
                pltpu.VMEM((rows, padded), f32),
                pltpu.VMEM((rows, padded), f32),
                pltpu.VMEM((rows, padded), f32),
                pltpu.VMEM((rows, padded), f32),
                pltpu.VMEM((rows, padded), f32),
                pltpu.VMEM((M, rows, padded), f32),
                pltpu.VMEM((M, rows, padded), f32),
                pltpu.VMEM((M, rows, padded), f32),
                pltpu.VMEM((rows, padded), f32),
                pltpu.VMEM((M, rows, cells), f32),
                pltpu.VMEM((3, rows, LANE), f32),
                pltpu.VMEM((slices, 8, LANE), f32),
                pltpu.VMEM((M, 8, LANE), f32),
                dma((2,)),
                dma, dma((chunks,)), dma, dma((chunks,)), dma, dma((chunks,)),
                dma, dma((chunks,)), dma, dma, pltpu.SemaphoreType.REGULAR((far,)),
                dma, dma, dma, dma, dma, dma, dma,
            ],
            compiler_params=pltpu.CompilerParams(
                collective_id=0, has_side_effects=True, vmem_limit_bytes=48 * 1024 * 1024
            ),
        )(
            pltpu.with_memory_space_constraint(slice_starts, pltpu.HBM),
            pltpu.with_memory_space_constraint(coupling, pltpu.HBM),
        )
        return tuple(
            pl.pallas_call(
                unload,
                out_shape=(pltpu.HBM(values.shape, f32), pltpu.HBM(logs.shape, f32)),
                in_specs=[anyplace, anyplace],
                out_specs=(anywhere, anywhere),
                scratch_shapes=[dma((PIECES + 1,))],
                compiler_params=pltpu.CompilerParams(vmem_limit_bytes=1024 * 1024),
            )(values, logs)
        )

    return jax.shard_map(
        body,
        mesh=mesh,
        in_specs=(P("tm", None, None), P()),
        out_specs=(P("tm", "node", None, None), P()),
        check_vma=False,
    )
```

```python
import functools
import jax
import jax.numpy as jnp
from jax import lax
from jax.experimental import pallas as pl
from jax.experimental.pallas import tpu as pltpu
from jax.sharding import PartitionSpec as P

M = 4
STEP = 16
FIRST = (4, 8, 12)
SLANT = 2
KINDS = (1, 1, 1, 2, 0, 1, 2, 0, 1, 2, 0)
START = (("even", 3), ("odd", 4), ("across", 1), ("ahead", 1), ("even", 4), ("across", 2), ("ahead", 2), ("even", 5), ("odd", 5), ("across", 3))
STEADY = ((0, "odd", 6), (1, "ahead", 3), (1, "even", 6), (2, "across", 5), (3, "back", 3))
EARLY = {(0, 0): (("odd", 6),), (0, 1): (("even", 6),), (0, 2): (("across", 4),), (1, 0): (("odd", 7),), (1, 1): (("ahead", 3), ("even", 7)), (1, 2): (("across", 5),), (1, 3): (("ahead", 4), ("back", 3))}
SETTLED = 2
REST = 16
LANE = 128
HALO = 3
PAD = 4
PIECES = 1
MESH = pl.DeviceIdType.MESH

time_step = 0.5
log_floor = 0.05


def legendre_gap(point, node_count):
    before = 1.0
    current = point
    for degree in range(1, node_count):
        following = ((2 * degree + 1) * point * current - degree * before) / (degree + 1)
        before = current
        current = following
    return current - before


def collocation(node_count):
    points = []
    samples = 4000
    for sample_index in range(samples - 1):
        lower_end = -1.0 + 2.0 * sample_index / samples
        upper_end = -1.0 + 2.0 * (sample_index + 1) / samples
        lower_value = legendre_gap(lower_end, node_count)
        upper_value = legendre_gap(upper_end, node_count)
        if lower_value * upper_value < 0.0:
            for halving in range(80):
                middle = 0.5 * (lower_end + upper_end)
                middle_value = legendre_gap(middle, node_count)
                if lower_value * middle_value <= 0.0:
                    upper_end = middle
                else:
                    lower_end = middle
                    lower_value = middle_value
            points.append(0.5 * (lower_end + upper_end))
    points.append(1.0)
    node_times = [(point + 1.0) / 2.0 for point in points]
    matrix = [[0.0] * node_count for row_index in range(node_count)]
    for column in range(node_count):
        coeffs = [1.0]
        for other in range(node_count):
            if other != column:
                scale = node_times[column] - node_times[other]
                shifted = [0.0] + coeffs
                scaled = [value * node_times[other] for value in coeffs] + [0.0]
                coeffs = [(shifted[power] - scaled[power]) / scale for power in range(len(shifted))]
        for row_index in range(node_count):
            upper_time = node_times[row_index]
            matrix[row_index][column] = sum(
                (
                    coeffs[power] * upper_time ** (power + 1) / (power + 1)
                    for power in range(len(coeffs))
                )
            )
    return (node_times, matrix)


def plan(tiles):
    bounds = [0]
    for size in FIRST:
        bounds.append(bounds[-1] + size)
    while bounds[-1] < tiles:
        bounds.append(min(bounds[-1] + REST, tiles))
    return bounds


def kernel(
    slices, rows, cells,
    start_hbm, coupling_hbm, out_hbm, log_ref,
    log_tile, log_sem,
    own, couple, prev1, prev2, prev3, relay, here, there, mid, before, result,
    acc, parts,
    load_sem, s_prev1, r_prev1, s_prev2, r_prev2, s_prev3, r_prev3,
    s_relay, r_relay, s_side, s_diag, far,
    s_out, r_out, local_sem, s_log, r_log,
):
    p = lax.axis_index("tm")
    n = lax.axis_index("node")
    all_tiles = cells // LANE
    bounds = plan(all_tiles)
    chunks = len(bounds) - 1
    my_rows = pl.ds(pl.multiple_of(n * rows, rows), rows)
    node_times, matrix = collocation(M)
    weight = [[time_step * value for value in line] for line in matrix]
    implicit = [time_step * moment / M for moment in node_times]
    even = lax.rem(p, 2) == 0
    first = p == 0
    second = p == 1

    loads = []
    for index, (source, target) in enumerate(
        ((start_hbm.at[0, my_rows], own), (coupling_hbm.at[my_rows], couple))
    ):
        for piece, (lo, to, size) in enumerate(
            ((0, PAD * LANE, cells), (cells - HALO * LANE, LANE, HALO * LANE), (0, PAD * LANE + cells, HALO * LANE))
        ):
            copy = pltpu.make_async_copy(
                source.at[:, pl.ds(lo, size)],
                target.at[:, pl.ds(to, size)],
                load_sem.at[index],
            )
            copy.start()
        whole = cells + 2 * HALO * LANE
        loads.append(
            pltpu.make_async_copy(
                target.at[:, pl.ds(0, whole)], target.at[:, pl.ds(0, whole)], load_sem.at[index]
            )
        )

    partner = jnp.where(even, p + 1, p - 1)
    ahead = lax.rem(p + 2, slices)
    behind = lax.rem(p + slices - 2, slices)
    has_behind = p >= 2
    has_ahead = p + 2 < slices
    odd = jnp.logical_not(even)
    along = has_behind.astype(jnp.int32) + has_ahead.astype(jnp.int32)
    slanted = jnp.where(even, has_behind, has_ahead)
    slant = jnp.where(even, lax.rem(p + slices - 1, slices), lax.rem(p + 1, slices))

    def signal(semaphore, tm, node):
        pl.semaphore_signal(
            semaphore, inc=1, device_id={"tm": tm, "node": node}, device_id_type=MESH
        )

    def signal_along(semaphore):
        @pl.when(has_behind)
        def _():
            signal(semaphore, behind, n)

        @pl.when(has_ahead)
        def _():
            signal(semaphore, ahead, n)

    barrier = pltpu.get_barrier_semaphore()
    signal_along(barrier)

    @pl.when(slanted)
    def _():
        signal(barrier, slant, n)

    signal(barrier, partner, n)
    for step in range(1, M):
        signal(barrier, p, lax.rem(n + step, M))
    pl.semaphore_wait(barrier, along + slanted.astype(jnp.int32) + M)
    rounds = max(slices // 2 - 2, 0)

    def meet(index):
        if 0 < index <= rounds:
            pl.semaphore_wait(far.at[index - 1], along)
        if index < rounds:
            signal_along(far.at[index])
        if index == rounds:
            signal(far.at[rounds], partner, n)
        if index == rounds + 1:
            pl.semaphore_wait(far.at[rounds], 1)
            for step in range(1, M):
                signal(far.at[rounds + 1], p, lax.rem(n + step, M))
        if index == rounds + 2:
            pl.semaphore_wait(far.at[rounds + 1], M - 1)

    meet(0)
    for copy in loads:
        copy.wait()

    def shape_of(count):
        return prev3.at[:, pl.ds(0, count * LANE)]

    def remote(source, target, send, recv, tm, node):
        return pltpu.make_async_remote_copy(
            src_ref=source, dst_ref=target, send_sem=send, recv_sem=recv,
            device_id={"tm": tm, "node": node}, device_id_type=MESH,
        )

    def part(ref, c):
        begin = (bounds[c] + HALO if c else -HALO) + PAD
        end = bounds[c + 1] + HALO + PAD
        return ref.at[:, pl.ds(begin * LANE, (end - begin) * LANE)]

    def to_partner_own(c):
        return remote(part(own, c), part(prev1, c), s_prev1, r_prev1.at[c], partner, n)

    def to_partner_forward(c):
        return remote(part(prev2, c), part(prev1, c), s_prev1, r_prev1.at[c], partner, n)

    def slant_own(c):
        return remote(part(own, c), part(prev1, c), s_diag, r_prev1.at[c], slant, n)

    def ahead_own(c):
        return remote(part(own, c), part(prev2, c), s_prev2, r_prev2.at[c], ahead, n)

    def ahead_forward(c):
        return remote(part(prev1, c), part(prev3, c), s_prev3, r_prev3.at[c], ahead, n)

    def relay_forward(c):
        return remote(part(prev2, c), part(relay, c), s_relay, r_relay.at[c], ahead, n)

    def to_partner_relayed(c):
        return remote(part(relay, c), part(prev3, c), s_side, r_prev3.at[c], partner, n)

    def to_partner_second(c):
        return remote(part(prev2, c), part(prev3, c), s_side, r_prev3.at[c], partner, n)

    def relayed(c):
        return KINDS[c % len(KINDS)] == 0

    def crossed(c):
        return KINDS[c % len(KINDS)] != 2

    def sends_third(c):
        if relayed(c):
            return None
        if crossed(c):
            return jnp.logical_and(has_ahead, jnp.logical_and(even, has_behind))
        return jnp.logical_and(has_ahead, jnp.logical_not(first))

    def start_even(c):
        @pl.when(even)
        def _():
            to_partner_own(c).start()

            @pl.when(has_ahead)
            def _():
                ahead_own(c).start()

    def start_odd(c):
        @pl.when(jnp.logical_and(odd, has_ahead))
        def _():
            if c < SLANT:
                slant_own(c).start()
            ahead_own(c).start()

    def pass_across(c):
        @pl.when(has_behind)
        def _():
            ahead_own(c).wait_recv()

        @pl.when(jnp.logical_and(odd, has_behind))
        def _():
            if c >= SLANT:
                to_partner_forward(c).start()
            if relayed(c):

                @pl.when(has_ahead)
                def _():
                    relay_forward(c).start()

        if crossed(c):

            @pl.when(jnp.logical_and(even, has_behind))
            def _():
                to_partner_second(c).start()

    def pass_back(c):
        if relayed(c):

            @pl.when(jnp.logical_and(odd, p >= 5))
            def _():
                relay_forward(c).wait_recv()
                to_partner_relayed(c).start()

    def pass_ahead(c):
        @pl.when(odd)
        def _():
            to_partner_own(c).wait_recv()

        @pl.when(jnp.logical_and(even, has_behind))
        def _():
            to_partner_forward(c).wait_recv()

        if not relayed(c):

            @pl.when(sends_third(c))
            def _():
                ahead_forward(c).start()

    acc[...] = jnp.zeros_like(acc)

    def diffusion(v, c, k):
        size = (k + 2) * LANE
        right = pltpu.roll(v, size - 1, 1)
        flux = c * (right - v)
        left = pltpu.roll(flux, 1, 1)
        return (flux - left)[:, LANE:LANE + k * LANE]

    def finish(d, top, target, a):
        dd = d * d
        tt = top * top
        above = target * (d * dd) + (2.0 * a) * (top * tt)
        below = d * ((1.0 - a) * dd + (3.0 * a) * tt)
        guess = pl.reciprocal(below, approx=True)
        return above * (guess * (2.0 - below * guess))

    def two_steps(base, defect, u, square, reaction, a):
        d = (3.0 * a) * square + (1.0 - a)
        return finish(d, defect + u * d, base - a * reaction, a)

    def equal_nodes(begin, vw, cw, k):
        v = vw[:, LANE:LANE + k * LANE]
        square = v * v
        reaction = v - v * square
        four = 4.0 * (diffusion(vw, cw, k) + reaction)
        slope = 3.0 * square - 1.0
        lift = four + v * slope
        pull = four - reaction

        def node(m):
            a = implicit[m]
            return finish(1.0 + a * slope, begin + a * lift, begin + a * pull, a)

        return v, four, node

    def folded(value, k):
        out = value[:, :LANE]
        for piece in range(1, k):
            out = out + value[:, piece * LANE:(piece + 1) * LANE]
        return out

    def run(begin, end, block, counted):
        count = (end - begin) // STEP

        def step(i, carry):
            block(begin + i * STEP, STEP, counted)
            return carry

        lax.fori_loop(0, count, step, 0)
        if begin + count * STEP < end:
            block(begin + count * STEP, end - begin - count * STEP, counted)

    def over(c, lag, block):
        begin = bounds[c] + lag if c else 0
        end = min(bounds[c + 1] + lag, all_tiles)
        if c == 0 and lag:
            block(-lag, lag, False)
        run(begin, end, block, True)
        if c == chunks - 1 and lag:
            block(all_tiles, lag, False)

    def lanes(offset):
        return offset * LANE if isinstance(offset, int) else pl.multiple_of(offset * LANE, LANE)

    def wide(tile, k):
        return pl.ds(lanes(tile + PAD - 1), (k + 2) * LANE)

    def centre(tile, k):
        return pl.ds(lanes(tile + PAD), k * LANE)

    begun = {"even": 0, "odd": 0, "across": 0, "ahead": 0, "back": 0}
    moves = {
        "even": start_even, "odd": start_odd,
        "across": pass_across, "ahead": pass_ahead, "back": pass_back,
    }

    def proceed(name, upto):
        for index in range(begun[name], min(upto, chunks)):
            moves[name](index)
        begun[name] = max(begun[name], upto)

    for name, upto in START:
        proceed(name, upto)

    def stage(k, place):
        for name, upto in EARLY.get((k, place), ()):
            proceed(name, upto)
        if k >= SETTLED:
            for at, name, lead in STEADY:
                if at == place:
                    proceed(name, k + lead)

    for c in range(chunks):
        base_lane = bounds[c] * LANE
        chunk = (bounds[c + 1] - bounds[c]) * LANE

        stage(c, 0)
        for name in moves:
            proceed(name, c + 1)

        @pl.when(p >= 3)
        def _():
            ahead_forward(c).wait_recv()

        def stage_a(tile, k, counted):
            middle = slice(LANE, LANE + k * LANE)
            cw = couple[:, wide(tile, k)]
            at = centre(tile, k)
            vw = own[:, wide(tile, k)]
            p1w = jnp.where(first, vw, prev1[:, wide(tile, k)])
            p1 = p1w[:, middle]
            p2w = jnp.where(p <= 1, p1w, prev2[:, wide(tile, k)])
            p2 = p2w[:, middle]
            p3 = jnp.where(p <= 2, p2, prev3[:, at])

            v, four, node = equal_nodes(p1, vw, cw, k)
            for m in range(M):
                here[m, :, at] = node(m)
            if counted:
                gap = p1 - v
                cross = 2.0 * sum(implicit)
                curve = sum(a * a for a in implicit)
                acc[0] += folded(
                    gap * (float(M) * gap + cross * four) + curve * (four * four), k
                )

            _, _, node = equal_nodes(p2, p1w, cw, k)
            for m in range(M):
                there[m, :, at] = node(m)

            _, _, node = equal_nodes(p3, p2w, cw, k)
            before[:, at] = jnp.where(second, p1, node(M - 1))

        over(c, 2, stage_a)
        stage(c, 1)

        def update(source, begin, cw, tile, k, which, counted):
            values = []
            forcings = []
            for m in range(M):
                vw = source[m, :, wide(tile, k)]
                v = vw[:, LANE:LANE + k * LANE]
                square = v * v
                reaction = v - v * square
                values.append((v, square, reaction))
                forcings.append(diffusion(vw, cw, k) + reaction)
            found = None
            outputs = []
            for m in range(M):
                base = begin
                for j in range(M):
                    base = base + weight[m][j] * forcings[j]
                v, square, reaction = values[m]
                defect = base - v
                if counted:
                    found = defect * defect if found is None else found + defect * defect
                outputs.append(two_steps(base, defect, v, square, reaction, implicit[m]))
            if counted:
                acc[which] += folded(found, k)
            return outputs

        def stage_b(tile, k, counted):
            cw = couple[:, wide(tile, k)]
            at = centre(tile, k)
            begin = jnp.where(first, own[:, centre(tile, k)], there[M - 1, :, at])
            outputs = update(here, begin, cw, tile, k, 1, counted)
            for m in range(M):
                mid[m, :, at] = outputs[m]
            mixed = None
            mixed_reaction = None
            for m in range(M):
                w = weight[M - 1][m]
                vw = there[m, :, wide(tile, k)]
                v = vw[:, LANE:LANE + k * LANE]
                square = v * v
                reaction = v - v * square
                mixed = w * vw if mixed is None else mixed + w * vw
                mixed_reaction = w * reaction if mixed_reaction is None else mixed_reaction + w * reaction
            base = before[:, at] + (diffusion(mixed, cw, k) + mixed_reaction)
            last = two_steps(base, base - v, v, square, reaction, implicit[M - 1])
            before[:, at] = jnp.where(first, own[:, centre(tile, k)], last)

        over(c, 1, stage_b)
        stage(c, 2)

        def stage_c(tile, k, counted):
            cw = couple[:, wide(tile, k)]
            outputs = update(mid, before[:, centre(tile, k)], cw, tile, k, 2, counted)
            at = pl.ds(lanes(tile), k * LANE)
            for m in range(M):
                result[m, :, at] = outputs[m]

        over(c, 0, stage_c)

        if c >= 2:
            meet(c - 1)
        here_cells = pl.ds(base_lane, chunk)
        target = out_hbm.at[0, 0, my_rows, here_cells]
        for step in (2, 3, 1):
            peer = lax.rem(n + step, M)
            remote(result.at[peer, :, here_cells], target, s_out, r_out, p, peer).start()
        pltpu.make_async_copy(result.at[n, :, here_cells], target, local_sem).start()
        stage(c, 3)

    for index in range(max(chunks - 1, 1), rounds + 3):
        meet(index)
    lane = lax.broadcasted_iota(jnp.int32, (rows, LANE), 1)
    sub = lax.broadcasted_iota(jnp.int32, (rows, LANE), 0)
    mixed = jnp.zeros((rows, LANE), jnp.float32)
    for which in range(3):
        per_system = jnp.sum(acc[which], axis=1, keepdims=True)
        place = which * M * rows + n * rows + sub
        mixed = mixed + jnp.where(lane == place, per_system, 0.0)
    slot = p * M + n
    parts[slot] = jnp.sum(mixed, axis=0, keepdims=True)
    for other in range(slices - 1, -1, -1):
        for step in range(M - 1, -1, -1):
            if other or step:
                remote(
                    parts.at[slot], parts.at[slot], s_log, r_log,
                    lax.rem(p + other, slices), lax.rem(n + step, M),
                ).start()
    others = parts.at[pl.ds(0, slices * M - 1)]
    gathered = remote(others, others, s_log, r_log, partner, n)
    gathered.wait_recv()
    summed = jnp.sum(parts[...], axis=0)
    logs = jnp.log(log_floor + summed / (slices * M * cells))
    for which in range(3):
        log_tile[which:which + 1, :] = logs[:, which * M * rows:(which + 1) * M * rows]
    log_copy = pltpu.make_async_copy(log_tile, log_ref, log_sem)
    log_copy.start()

    log_copy.wait()
    gathered.wait_send()
    three = result.at[pl.ds(0, M - 1)]
    outputs = remote(three, three, s_out, r_out, partner, n)
    outputs.wait_send()
    outputs.wait_recv()
    mine = result.at[0]
    pltpu.make_async_copy(mine, mine, local_sem).wait()

    def span(c):
        return bounds[c + 1] - bounds[c] + (0 if c else 2 * HALO)

    def drain(semaphore, wanted):
        count = sum(span(c) for c in range(chunks) if wanted(c))
        if count:
            remote(shape_of(count), shape_of(count), semaphore, r_prev3.at[0], partner, n).wait_send()

    def direct(c):
        return not relayed(c)

    def straight(c):
        return not crossed(c)

    @pl.when(has_ahead)
    def _():
        drain(s_prev2, lambda c: True)

    @pl.when(jnp.logical_and(has_ahead, jnp.logical_and(even, has_behind)))
    def _():
        drain(s_prev3, direct)

    @pl.when(jnp.logical_and(has_ahead, odd))
    def _():
        drain(s_prev3, straight)
        drain(s_diag, lambda c: c < SLANT)

    @pl.when(even)
    def _():
        drain(s_prev1, lambda c: True)

    @pl.when(jnp.logical_and(odd, has_behind))
    def _():
        drain(s_prev1, lambda c: c >= SLANT)

    @pl.when(jnp.logical_and(has_ahead, jnp.logical_and(odd, has_behind)))
    def _():
        drain(s_relay, relayed)

    @pl.when(jnp.logical_and(odd, p >= 5))
    def _():
        drain(s_side, relayed)

    @pl.when(jnp.logical_and(even, has_behind))
    def _():
        drain(s_side, crossed)


def unload(values, logs, values_hbm, logs_hbm, sem):
    size = values.shape[2] // PIECES
    copies = [pltpu.make_async_copy(logs, logs_hbm, sem.at[PIECES])]
    for piece in range(PIECES):
        at = pl.ds(piece * size, size)
        copies.append(
            pltpu.make_async_copy(values.at[:, :, at], values_hbm.at[:, :, at], sem.at[piece])
        )
    for copy in copies:
        copy.start()
    for copy in copies:
        copy.wait()


def solution(mesh):
    slices = mesh.shape["tm"]

    def body(slice_starts, coupling):
        systems, cells = coupling.shape
        rows = systems // M
        chunks = len(plan(cells // LANE)) - 1
        far = max(slices // 2 - 2, 0) + 2
        padded = cells + 2 * PAD * LANE
        f32 = jnp.float32
        dma = pltpu.SemaphoreType.DMA
        anyplace = pl.BlockSpec(memory_space=pl.ANY)
        anywhere = pl.BlockSpec(memory_space=pltpu.HBM)
        values, logs = pl.pallas_call(
            functools.partial(kernel, slices, rows, cells),
            out_shape=(
                jax.ShapeDtypeStruct((1, 1, systems, cells), f32),
                jax.ShapeDtypeStruct((3, systems), f32),
            ),
            in_specs=[anywhere, anywhere],
            out_specs=(anyplace, anyplace),
            scratch_shapes=[
                pltpu.VMEM((3, systems), f32), dma,
                pltpu.VMEM((rows, padded), f32),
                pltpu.VMEM((rows, padded), f32),
                pltpu.VMEM((rows, padded), f32),
                pltpu.VMEM((rows, padded), f32),
                pltpu.VMEM((rows, padded), f32),
                pltpu.VMEM((rows, padded), f32),
                pltpu.VMEM((M, rows, padded), f32),
                pltpu.VMEM((M, rows, padded), f32),
                pltpu.VMEM((M, rows, padded), f32),
                pltpu.VMEM((rows, padded), f32),
                pltpu.VMEM((M, rows, cells), f32),
                pltpu.VMEM((3, rows, LANE), f32),
                pltpu.VMEM((slices * M, 1, LANE), f32),
                dma((2,)),
                dma, dma((chunks,)), dma, dma((chunks,)), dma, dma((chunks,)),
                dma, dma((chunks,)), dma, dma, pltpu.SemaphoreType.REGULAR((far,)),
                dma, dma, dma, dma, dma,
            ],
            compiler_params=pltpu.CompilerParams(
                collective_id=0, has_side_effects=True, vmem_limit_bytes=48 * 1024 * 1024
            ),
        )(
            pltpu.with_memory_space_constraint(slice_starts, pltpu.HBM),
            pltpu.with_memory_space_constraint(coupling, pltpu.HBM),
        )
        return tuple(
            pl.pallas_call(
                unload,
                out_shape=(pltpu.HBM(values.shape, f32), pltpu.HBM(logs.shape, f32)),
                in_specs=[anyplace, anyplace],
                out_specs=(anywhere, anywhere),
                scratch_shapes=[dma((PIECES + 1,))],
                compiler_params=pltpu.CompilerParams(vmem_limit_bytes=1024 * 1024),
            )(values, logs)
        )

    return jax.shard_map(
        body,
        mesh=mesh,
        in_specs=(P("tm", None, None), P()),
        out_specs=(P("tm", "node", None, None), P()),
        check_vma=False,
    )
```

```python
import functools
import jax
import jax.numpy as jnp
from jax import lax
from jax.experimental import pallas as pl
from jax.experimental.pallas import tpu as pltpu
from jax.sharding import PartitionSpec as P

M = 4
STEP = 16
FIRST = (6, 10, 16)
SLANT = 2
KINDS = (1, 1, 1, 2, 0, 1, 2, 0, 1, 2, 0)
START = (("even", 3), ("odd", 4), ("across", 1), ("ahead", 1), ("even", 4), ("across", 2), ("ahead", 2), ("even", 5), ("odd", 5), ("across", 3))
STEADY = ((0, "odd", 6), (1, "ahead", 3), (1, "even", 6), (2, "across", 5), (3, "back", 3))
EARLY = {(0, 0): (("odd", 6),), (0, 1): (("even", 6),), (0, 2): (("across", 4),), (1, 0): (("odd", 7),), (1, 1): (("ahead", 3), ("even", 7)), (1, 2): (("across", 5),), (1, 3): (("ahead", 4), ("back", 3))}
SETTLED = 2
REST = 16
LANE = 128
HALO = 3
PAD = 4
PIECES = 1
MESH = pl.DeviceIdType.MESH

time_step = 0.5
log_floor = 0.05


def legendre_gap(point, node_count):
    before = 1.0
    current = point
    for degree in range(1, node_count):
        following = ((2 * degree + 1) * point * current - degree * before) / (degree + 1)
        before = current
        current = following
    return current - before


def collocation(node_count):
    points = []
    samples = 4000
    for sample_index in range(samples - 1):
        lower_end = -1.0 + 2.0 * sample_index / samples
        upper_end = -1.0 + 2.0 * (sample_index + 1) / samples
        lower_value = legendre_gap(lower_end, node_count)
        upper_value = legendre_gap(upper_end, node_count)
        if lower_value * upper_value < 0.0:
            for halving in range(80):
                middle = 0.5 * (lower_end + upper_end)
                middle_value = legendre_gap(middle, node_count)
                if lower_value * middle_value <= 0.0:
                    upper_end = middle
                else:
                    lower_end = middle
                    lower_value = middle_value
            points.append(0.5 * (lower_end + upper_end))
    points.append(1.0)
    node_times = [(point + 1.0) / 2.0 for point in points]
    matrix = [[0.0] * node_count for row_index in range(node_count)]
    for column in range(node_count):
        coeffs = [1.0]
        for other in range(node_count):
            if other != column:
                scale = node_times[column] - node_times[other]
                shifted = [0.0] + coeffs
                scaled = [value * node_times[other] for value in coeffs] + [0.0]
                coeffs = [(shifted[power] - scaled[power]) / scale for power in range(len(shifted))]
        for row_index in range(node_count):
            upper_time = node_times[row_index]
            matrix[row_index][column] = sum(
                (
                    coeffs[power] * upper_time ** (power + 1) / (power + 1)
                    for power in range(len(coeffs))
                )
            )
    return (node_times, matrix)


def plan(tiles):
    bounds = [0]
    for size in FIRST:
        bounds.append(bounds[-1] + size)
    while bounds[-1] < tiles:
        bounds.append(min(bounds[-1] + REST, tiles))
    return bounds


def kernel(
    slices, rows, cells,
    start_hbm, coupling_hbm, out_hbm, log_ref,
    log_tile, log_sem,
    own, couple, prev1, prev2, prev3, relay, here, there, mid, before, result,
    acc, parts,
    load_sem, s_prev1, r_prev1, s_prev2, r_prev2, s_prev3, r_prev3,
    s_relay, r_relay, s_side, s_diag, far,
    s_out, r_out, local_sem, s_log, r_log,
):
    p = lax.axis_index("tm")
    n = lax.axis_index("node")
    all_tiles = cells // LANE
    bounds = plan(all_tiles)
    chunks = len(bounds) - 1
    my_rows = pl.ds(pl.multiple_of(n * rows, rows), rows)
    node_times, matrix = collocation(M)
    weight = [[time_step * value for value in line] for line in matrix]
    implicit = [time_step * moment / M for moment in node_times]
    even = lax.rem(p, 2) == 0
    first = p == 0
    second = p == 1

    loads = []
    for index, (source, target) in enumerate(
        ((start_hbm.at[0, my_rows], own), (coupling_hbm.at[my_rows], couple))
    ):
        for piece, (lo, to, size) in enumerate(
            ((0, PAD * LANE, cells), (cells - HALO * LANE, LANE, HALO * LANE), (0, PAD * LANE + cells, HALO * LANE))
        ):
            copy = pltpu.make_async_copy(
                source.at[:, pl.ds(lo, size)],
                target.at[:, pl.ds(to, size)],
                load_sem.at[index],
            )
            copy.start()
        whole = cells + 2 * HALO * LANE
        loads.append(
            pltpu.make_async_copy(
                target.at[:, pl.ds(0, whole)], target.at[:, pl.ds(0, whole)], load_sem.at[index]
            )
        )

    partner = jnp.where(even, p + 1, p - 1)
    ahead = lax.rem(p + 2, slices)
    behind = lax.rem(p + slices - 2, slices)
    has_behind = p >= 2
    has_ahead = p + 2 < slices
    odd = jnp.logical_not(even)
    along = has_behind.astype(jnp.int32) + has_ahead.astype(jnp.int32)
    slanted = jnp.where(even, has_behind, has_ahead)
    slant = jnp.where(even, lax.rem(p + slices - 1, slices), lax.rem(p + 1, slices))

    def signal(semaphore, tm, node):
        pl.semaphore_signal(
            semaphore, inc=1, device_id={"tm": tm, "node": node}, device_id_type=MESH
        )

    def signal_along(semaphore):
        @pl.when(has_behind)
        def _():
            signal(semaphore, behind, n)

        @pl.when(has_ahead)
        def _():
            signal(semaphore, ahead, n)

    barrier = pltpu.get_barrier_semaphore()
    signal_along(barrier)

    @pl.when(slanted)
    def _():
        signal(barrier, slant, n)

    signal(barrier, partner, n)
    for step in range(1, M):
        signal(barrier, p, lax.rem(n + step, M))
    pl.semaphore_wait(barrier, along + slanted.astype(jnp.int32) + M)
    rounds = max(slices // 2 - 2, 0)

    def meet(index):
        if 0 < index <= rounds:
            pl.semaphore_wait(far.at[index - 1], along)
        if index < rounds:
            signal_along(far.at[index])
        if index == rounds:
            signal(far.at[rounds], partner, n)
        if index == rounds + 1:
            pl.semaphore_wait(far.at[rounds], 1)
            for step in range(1, M):
                signal(far.at[rounds + 1], p, lax.rem(n + step, M))
        if index == rounds + 2:
            pl.semaphore_wait(far.at[rounds + 1], M - 1)

    meet(0)
    for copy in loads:
        copy.wait()

    def shape_of(count):
        return prev3.at[:, pl.ds(0, count * LANE)]

    def remote(source, target, send, recv, tm, node):
        return pltpu.make_async_remote_copy(
            src_ref=source, dst_ref=target, send_sem=send, recv_sem=recv,
            device_id={"tm": tm, "node": node}, device_id_type=MESH,
        )

    def part(ref, c):
        begin = (bounds[c] + HALO if c else -HALO) + PAD
        end = bounds[c + 1] + HALO + PAD
        return ref.at[:, pl.ds(begin * LANE, (end - begin) * LANE)]

    def to_partner_own(c):
        return remote(part(own, c), part(prev1, c), s_prev1, r_prev1.at[c], partner, n)

    def to_partner_forward(c):
        return remote(part(prev2, c), part(prev1, c), s_prev1, r_prev1.at[c], partner, n)

    def slant_own(c):
        return remote(part(own, c), part(prev1, c), s_diag, r_prev1.at[c], slant, n)

    def ahead_own(c):
        return remote(part(own, c), part(prev2, c), s_prev2, r_prev2.at[c], ahead, n)

    def ahead_forward(c):
        return remote(part(prev1, c), part(prev3, c), s_prev3, r_prev3.at[c], ahead, n)

    def relay_forward(c):
        return remote(part(prev2, c), part(relay, c), s_relay, r_relay.at[c], ahead, n)

    def to_partner_relayed(c):
        return remote(part(relay, c), part(prev3, c), s_side, r_prev3.at[c], partner, n)

    def to_partner_second(c):
        return remote(part(prev2, c), part(prev3, c), s_side, r_prev3.at[c], partner, n)

    def relayed(c):
        return KINDS[c % len(KINDS)] == 0

    def crossed(c):
        return KINDS[c % len(KINDS)] != 2

    def sends_third(c):
        if relayed(c):
            return None
        if crossed(c):
            return jnp.logical_and(has_ahead, jnp.logical_and(even, has_behind))
        return jnp.logical_and(has_ahead, jnp.logical_not(first))

    def start_even(c):
        @pl.when(even)
        def _():
            to_partner_own(c).start()

            @pl.when(has_ahead)
            def _():
                ahead_own(c).start()

    def start_odd(c):
        @pl.when(jnp.logical_and(odd, has_ahead))
        def _():
            if c < SLANT:
                slant_own(c).start()
            ahead_own(c).start()

    def pass_across(c):
        @pl.when(has_behind)
        def _():
            ahead_own(c).wait_recv()

        @pl.when(jnp.logical_and(odd, has_behind))
        def _():
            if c >= SLANT:
                to_partner_forward(c).start()
            if relayed(c):

                @pl.when(has_ahead)
                def _():
                    relay_forward(c).start()

        if crossed(c):

            @pl.when(jnp.logical_and(even, has_behind))
            def _():
                to_partner_second(c).start()

    def pass_back(c):
        if relayed(c):

            @pl.when(jnp.logical_and(odd, p >= 5))
            def _():
                relay_forward(c).wait_recv()
                to_partner_relayed(c).start()

    def pass_ahead(c):
        @pl.when(odd)
        def _():
            to_partner_own(c).wait_recv()

        @pl.when(jnp.logical_and(even, has_behind))
        def _():
            to_partner_forward(c).wait_recv()

        if not relayed(c):

            @pl.when(sends_third(c))
            def _():
                ahead_forward(c).start()

    acc[...] = jnp.zeros_like(acc)

    def diffusion(v, c, k):
        size = (k + 2) * LANE
        right = pltpu.roll(v, size - 1, 1)
        flux = c * (right - v)
        left = pltpu.roll(flux, 1, 1)
        return (flux - left)[:, LANE:LANE + k * LANE]

    def finish(d, top, target, a):
        dd = d * d
        tt = top * top
        above = target * (d * dd) + (2.0 * a) * (top * tt)
        below = d * ((1.0 - a) * dd + (3.0 * a) * tt)
        guess = pl.reciprocal(below, approx=True)
        return above * (guess * (2.0 - below * guess))

    def two_steps(base, defect, u, square, reaction, a):
        d = (3.0 * a) * square + (1.0 - a)
        return finish(d, defect + u * d, base - a * reaction, a)

    def equal_nodes(begin, vw, cw, k):
        v = vw[:, LANE:LANE + k * LANE]
        square = v * v
        reaction = v - v * square
        four = 4.0 * (diffusion(vw, cw, k) + reaction)
        slope = 3.0 * square - 1.0
        lift = four + v * slope
        pull = four - reaction

        def node(m):
            a = implicit[m]
            return finish(1.0 + a * slope, begin + a * lift, begin + a * pull, a)

        return v, four, node

    def folded(value, k):
        out = value[:, :LANE]
        for piece in range(1, k):
            out = out + value[:, piece * LANE:(piece + 1) * LANE]
        return out

    def run(begin, end, block, counted):
        count = (end - begin) // STEP

        def step(i, carry):
            block(begin + i * STEP, STEP, counted)
            return carry

        lax.fori_loop(0, count, step, 0)
        if begin + count * STEP < end:
            block(begin + count * STEP, end - begin - count * STEP, counted)

    def over(c, lag, block):
        begin = bounds[c] + lag if c else 0
        end = min(bounds[c + 1] + lag, all_tiles)
        if c == 0 and lag:
            block(-lag, lag, False)
        run(begin, end, block, True)
        if c == chunks - 1 and lag:
            block(all_tiles, lag, False)

    def lanes(offset):
        return offset * LANE if isinstance(offset, int) else pl.multiple_of(offset * LANE, LANE)

    def wide(tile, k):
        return pl.ds(lanes(tile + PAD - 1), (k + 2) * LANE)

    def centre(tile, k):
        return pl.ds(lanes(tile + PAD), k * LANE)

    begun = {"even": 0, "odd": 0, "across": 0, "ahead": 0, "back": 0}
    moves = {
        "even": start_even, "odd": start_odd,
        "across": pass_across, "ahead": pass_ahead, "back": pass_back,
    }

    def proceed(name, upto):
        for index in range(begun[name], min(upto, chunks)):
            moves[name](index)
        begun[name] = max(begun[name], upto)

    for name, upto in START:
        proceed(name, upto)

    def stage(k, place):
        for name, upto in EARLY.get((k, place), ()):
            proceed(name, upto)
        if k >= SETTLED:
            for at, name, lead in STEADY:
                if at == place:
                    proceed(name, k + lead)

    for c in range(chunks):
        base_lane = bounds[c] * LANE
        chunk = (bounds[c + 1] - bounds[c]) * LANE

        stage(c, 0)
        for name in moves:
            proceed(name, c + 1)

        @pl.when(p >= 3)
        def _():
            ahead_forward(c).wait_recv()

        def stage_a(tile, k, counted):
            middle = slice(LANE, LANE + k * LANE)
            cw = couple[:, wide(tile, k)]
            at = centre(tile, k)
            vw = own[:, wide(tile, k)]
            p1w = jnp.where(first, vw, prev1[:, wide(tile, k)])
            p1 = p1w[:, middle]
            p2w = jnp.where(p <= 1, p1w, prev2[:, wide(tile, k)])
            p2 = p2w[:, middle]
            p3 = jnp.where(p <= 2, p2, prev3[:, at])

            v, four, node = equal_nodes(p1, vw, cw, k)
            for m in range(M):
                here[m, :, at] = node(m)
            if counted:
                gap = p1 - v
                cross = 2.0 * sum(implicit)
                curve = sum(a * a for a in implicit)
                acc[0] += folded(
                    gap * (float(M) * gap + cross * four) + curve * (four * four), k
                )

            _, _, node = equal_nodes(p2, p1w, cw, k)
            for m in range(M):
                there[m, :, at] = node(m)

            _, _, node = equal_nodes(p3, p2w, cw, k)
            before[:, at] = jnp.where(second, p1, node(M - 1))

        over(c, 2, stage_a)
        stage(c, 1)

        def update(source, begin, cw, tile, k, which, counted):
            values = []
            forcings = []
            for m in range(M):
                vw = source[m, :, wide(tile, k)]
                v = vw[:, LANE:LANE + k * LANE]
                square = v * v
                reaction = v - v * square
                values.append((v, square, reaction))
                forcings.append(diffusion(vw, cw, k) + reaction)
            found = None
            outputs = []
            for m in range(M):
                base = begin
                for j in range(M):
                    base = base + weight[m][j] * forcings[j]
                v, square, reaction = values[m]
                defect = base - v
                if counted:
                    found = defect * defect if found is None else found + defect * defect
                outputs.append(two_steps(base, defect, v, square, reaction, implicit[m]))
            if counted:
                acc[which] += folded(found, k)
            return outputs

        def stage_b(tile, k, counted):
            cw = couple[:, wide(tile, k)]
            at = centre(tile, k)
            begin = jnp.where(first, own[:, centre(tile, k)], there[M - 1, :, at])
            outputs = update(here, begin, cw, tile, k, 1, counted)
            for m in range(M):
                mid[m, :, at] = outputs[m]
            mixed = None
            mixed_reaction = None
            for m in range(M):
                w = weight[M - 1][m]
                vw = there[m, :, wide(tile, k)]
                v = vw[:, LANE:LANE + k * LANE]
                square = v * v
                reaction = v - v * square
                mixed = w * vw if mixed is None else mixed + w * vw
                mixed_reaction = w * reaction if mixed_reaction is None else mixed_reaction + w * reaction
            base = before[:, at] + (diffusion(mixed, cw, k) + mixed_reaction)
            last = two_steps(base, base - v, v, square, reaction, implicit[M - 1])
            before[:, at] = jnp.where(first, own[:, centre(tile, k)], last)

        over(c, 1, stage_b)
        stage(c, 2)

        def stage_c(tile, k, counted):
            cw = couple[:, wide(tile, k)]
            outputs = update(mid, before[:, centre(tile, k)], cw, tile, k, 2, counted)
            at = pl.ds(lanes(tile), k * LANE)
            for m in range(M):
                result[m, :, at] = outputs[m]

        over(c, 0, stage_c)

        if c >= 2:
            meet(c - 1)
        here_cells = pl.ds(base_lane, chunk)
        target = out_hbm.at[0, 0, my_rows, here_cells]
        for step in (2, 3, 1):
            peer = lax.rem(n + step, M)
            remote(result.at[peer, :, here_cells], target, s_out, r_out, p, peer).start()
        pltpu.make_async_copy(result.at[n, :, here_cells], target, local_sem).start()
        stage(c, 3)

    for index in range(max(chunks - 1, 1), rounds + 3):
        meet(index)
    lane = lax.broadcasted_iota(jnp.int32, (rows, LANE), 1)
    sub = lax.broadcasted_iota(jnp.int32, (rows, LANE), 0)
    mixed = jnp.zeros((rows, LANE), jnp.float32)
    for which in range(3):
        per_system = jnp.sum(acc[which], axis=1, keepdims=True)
        place = which * M * rows + n * rows + sub
        mixed = mixed + jnp.where(lane == place, per_system, 0.0)
    slot = p * M + n
    parts[slot] = jnp.sum(mixed, axis=0, keepdims=True)
    for other in range(slices - 1, -1, -1):
        for step in range(M - 1, -1, -1):
            if other or step:
                remote(
                    parts.at[slot], parts.at[slot], s_log, r_log,
                    lax.rem(p + other, slices), lax.rem(n + step, M),
                ).start()
    others = parts.at[pl.ds(0, slices * M - 1)]
    gathered = remote(others, others, s_log, r_log, partner, n)
    gathered.wait_recv()
    summed = jnp.sum(parts[...], axis=0)
    logs = jnp.log(log_floor + summed / (slices * M * cells))
    for which in range(3):
        log_tile[which:which + 1, :] = logs[:, which * M * rows:(which + 1) * M * rows]
    log_copy = pltpu.make_async_copy(log_tile, log_ref, log_sem)
    log_copy.start()

    log_copy.wait()
    gathered.wait_send()
    three = result.at[pl.ds(0, M - 1)]
    outputs = remote(three, three, s_out, r_out, partner, n)
    outputs.wait_send()
    outputs.wait_recv()
    mine = result.at[0]
    pltpu.make_async_copy(mine, mine, local_sem).wait()

    def span(c):
        return bounds[c + 1] - bounds[c] + (0 if c else 2 * HALO)

    def drain(semaphore, wanted):
        count = sum(span(c) for c in range(chunks) if wanted(c))
        if count:
            remote(shape_of(count), shape_of(count), semaphore, r_prev3.at[0], partner, n).wait_send()

    def direct(c):
        return not relayed(c)

    def straight(c):
        return not crossed(c)

    @pl.when(has_ahead)
    def _():
        drain(s_prev2, lambda c: True)

    @pl.when(jnp.logical_and(has_ahead, jnp.logical_and(even, has_behind)))
    def _():
        drain(s_prev3, direct)

    @pl.when(jnp.logical_and(has_ahead, odd))
    def _():
        drain(s_prev3, straight)
        drain(s_diag, lambda c: c < SLANT)

    @pl.when(even)
    def _():
        drain(s_prev1, lambda c: True)

    @pl.when(jnp.logical_and(odd, has_behind))
    def _():
        drain(s_prev1, lambda c: c >= SLANT)

    @pl.when(jnp.logical_and(has_ahead, jnp.logical_and(odd, has_behind)))
    def _():
        drain(s_relay, relayed)

    @pl.when(jnp.logical_and(odd, p >= 5))
    def _():
        drain(s_side, relayed)

    @pl.when(jnp.logical_and(even, has_behind))
    def _():
        drain(s_side, crossed)


def unload(values, logs, values_hbm, logs_hbm, sem):
    size = values.shape[2] // PIECES
    copies = [pltpu.make_async_copy(logs, logs_hbm, sem.at[PIECES])]
    for piece in range(PIECES):
        at = pl.ds(piece * size, size)
        copies.append(
            pltpu.make_async_copy(values.at[:, :, at], values_hbm.at[:, :, at], sem.at[piece])
        )
    for copy in copies:
        copy.start()
    for copy in copies:
        copy.wait()


def solution(mesh):
    slices = mesh.shape["tm"]

    def body(slice_starts, coupling):
        systems, cells = coupling.shape
        rows = systems // M
        chunks = len(plan(cells // LANE)) - 1
        far = max(slices // 2 - 2, 0) + 2
        padded = cells + 2 * PAD * LANE
        f32 = jnp.float32
        dma = pltpu.SemaphoreType.DMA
        anyplace = pl.BlockSpec(memory_space=pl.ANY)
        anywhere = pl.BlockSpec(memory_space=pltpu.HBM)
        values, logs = pl.pallas_call(
            functools.partial(kernel, slices, rows, cells),
            out_shape=(
                jax.ShapeDtypeStruct((1, 1, systems, cells), f32),
                jax.ShapeDtypeStruct((3, systems), f32),
            ),
            in_specs=[anywhere, anywhere],
            out_specs=(anyplace, anyplace),
            scratch_shapes=[
                pltpu.VMEM((3, systems), f32), dma,
                pltpu.VMEM((rows, padded), f32),
                pltpu.VMEM((rows, padded), f32),
                pltpu.VMEM((rows, padded), f32),
                pltpu.VMEM((rows, padded), f32),
                pltpu.VMEM((rows, padded), f32),
                pltpu.VMEM((rows, padded), f32),
                pltpu.VMEM((M, rows, padded), f32),
                pltpu.VMEM((M, rows, padded), f32),
                pltpu.VMEM((M, rows, padded), f32),
                pltpu.VMEM((rows, padded), f32),
                pltpu.VMEM((M, rows, cells), f32),
                pltpu.VMEM((3, rows, LANE), f32),
                pltpu.VMEM((slices * M, 1, LANE), f32),
                dma((2,)),
                dma, dma((chunks,)), dma, dma((chunks,)), dma, dma((chunks,)),
                dma, dma((chunks,)), dma, dma, pltpu.SemaphoreType.REGULAR((far,)),
                dma, dma, dma, dma, dma,
            ],
            compiler_params=pltpu.CompilerParams(
                collective_id=0, has_side_effects=True, vmem_limit_bytes=48 * 1024 * 1024
            ),
        )(
            pltpu.with_memory_space_constraint(slice_starts, pltpu.HBM),
            pltpu.with_memory_space_constraint(coupling, pltpu.HBM),
        )
        return tuple(
            pl.pallas_call(
                unload,
                out_shape=(pltpu.HBM(values.shape, f32), pltpu.HBM(logs.shape, f32)),
                in_specs=[anyplace, anyplace],
                out_specs=(anywhere, anywhere),
                scratch_shapes=[dma((PIECES + 1,))],
                compiler_params=pltpu.CompilerParams(vmem_limit_bytes=1024 * 1024),
            )(values, logs)
        )

    return jax.shard_map(
        body,
        mesh=mesh,
        in_specs=(P("tm", None, None), P()),
        out_specs=(P("tm", "node", None, None), P()),
        check_vma=False,
    )
```

```python
import functools
import jax
import jax.numpy as jnp
from jax import lax
from jax.experimental import pallas as pl
from jax.experimental.pallas import tpu as pltpu
from jax.sharding import PartitionSpec as P

M = 4
STEP = 16
FIRST = (6, 10, 16)
SLANT = 2
KINDS = (1, 1, 1, 2, 0, 1, 2, 0, 1, 2, 0)
START = (("even", 3), ("odd", 4), ("across", 1), ("ahead", 1), ("even", 4), ("across", 2), ("ahead", 2), ("even", 5), ("odd", 5), ("across", 3))
STEADY = ((0, "odd", 6), (1, "ahead", 3), (1, "even", 6), (2, "across", 5), (3, "back", 3))
EARLY = {(0, 0): (("odd", 6),), (0, 1): (("even", 6),), (0, 2): (("across", 4),), (1, 0): (("odd", 7),), (1, 1): (("ahead", 3), ("even", 7)), (1, 2): (("across", 5),), (1, 3): (("ahead", 4), ("back", 3))}
SETTLED = 2
REST = 16
LANE = 128
HALO = 3
PAD = 4
PIECES = 1
MESH = pl.DeviceIdType.MESH

time_step = 0.5
log_floor = 0.05


def legendre_gap(point, node_count):
    before = 1.0
    current = point
    for degree in range(1, node_count):
        following = ((2 * degree + 1) * point * current - degree * before) / (degree + 1)
        before = current
        current = following
    return current - before


def collocation(node_count):
    points = []
    samples = 4000
    for sample_index in range(samples - 1):
        lower_end = -1.0 + 2.0 * sample_index / samples
        upper_end = -1.0 + 2.0 * (sample_index + 1) / samples
        lower_value = legendre_gap(lower_end, node_count)
        upper_value = legendre_gap(upper_end, node_count)
        if lower_value * upper_value < 0.0:
            for halving in range(80):
                middle = 0.5 * (lower_end + upper_end)
                middle_value = legendre_gap(middle, node_count)
                if lower_value * middle_value <= 0.0:
                    upper_end = middle
                else:
                    lower_end = middle
                    lower_value = middle_value
            points.append(0.5 * (lower_end + upper_end))
    points.append(1.0)
    node_times = [(point + 1.0) / 2.0 for point in points]
    matrix = [[0.0] * node_count for row_index in range(node_count)]
    for column in range(node_count):
        coeffs = [1.0]
        for other in range(node_count):
            if other != column:
                scale = node_times[column] - node_times[other]
                shifted = [0.0] + coeffs
                scaled = [value * node_times[other] for value in coeffs] + [0.0]
                coeffs = [(shifted[power] - scaled[power]) / scale for power in range(len(shifted))]
        for row_index in range(node_count):
            upper_time = node_times[row_index]
            matrix[row_index][column] = sum(
                (
                    coeffs[power] * upper_time ** (power + 1) / (power + 1)
                    for power in range(len(coeffs))
                )
            )
    return (node_times, matrix)


def plan(tiles):
    bounds = [0]
    for size in FIRST:
        bounds.append(bounds[-1] + size)
    while bounds[-1] < tiles:
        bounds.append(min(bounds[-1] + REST, tiles))
    return bounds


def kernel(
    slices, rows, cells,
    start_hbm, coupling_hbm, out_hbm, log_ref,
    log_tile, log_sem,
    own, couple, prev1, prev2, prev3, relay, here, there, mid, before, result,
    acc, parts,
    load_sem, s_prev1, r_prev1, s_prev2, r_prev2, s_prev3, r_prev3,
    s_relay, r_relay, s_side, s_diag, far,
    s_out, r_out, local_sem, s_log, r_log,
):
    p = lax.axis_index("tm")
    n = lax.axis_index("node")
    all_tiles = cells // LANE
    bounds = plan(all_tiles)
    chunks = len(bounds) - 1
    my_rows = pl.ds(pl.multiple_of(n * rows, rows), rows)
    node_times, matrix = collocation(M)
    weight = [[time_step * value for value in line] for line in matrix]
    implicit = [time_step * moment / M for moment in node_times]
    even = lax.rem(p, 2) == 0
    first = p == 0
    second = p == 1

    loads = []
    for index, (source, target) in enumerate(
        ((start_hbm.at[0, my_rows], own), (coupling_hbm.at[my_rows], couple))
    ):
        for piece, (lo, to, size) in enumerate(
            ((0, PAD * LANE, cells), (cells - HALO * LANE, LANE, HALO * LANE), (0, PAD * LANE + cells, HALO * LANE))
        ):
            copy = pltpu.make_async_copy(
                source.at[:, pl.ds(lo, size)],
                target.at[:, pl.ds(to, size)],
                load_sem.at[index],
            )
            copy.start()
        whole = cells + 2 * HALO * LANE
        loads.append(
            pltpu.make_async_copy(
                target.at[:, pl.ds(0, whole)], target.at[:, pl.ds(0, whole)], load_sem.at[index]
            )
        )

    partner = jnp.where(even, p + 1, p - 1)
    ahead = lax.rem(p + 2, slices)
    behind = lax.rem(p + slices - 2, slices)
    has_behind = p >= 2
    has_ahead = p + 2 < slices
    odd = jnp.logical_not(even)
    along = has_behind.astype(jnp.int32) + has_ahead.astype(jnp.int32)
    slanted = jnp.where(even, has_behind, has_ahead)
    slant = jnp.where(even, lax.rem(p + slices - 1, slices), lax.rem(p + 1, slices))

    def signal(semaphore, tm, node):
        pl.semaphore_signal(
            semaphore, inc=1, device_id={"tm": tm, "node": node}, device_id_type=MESH
        )

    def signal_along(semaphore):
        @pl.when(has_behind)
        def _():
            signal(semaphore, behind, n)

        @pl.when(has_ahead)
        def _():
            signal(semaphore, ahead, n)

    barrier = pltpu.get_barrier_semaphore()
    signal_along(barrier)

    @pl.when(slanted)
    def _():
        signal(barrier, slant, n)

    signal(barrier, partner, n)
    for step in range(1, M):
        signal(barrier, p, lax.rem(n + step, M))
    pl.semaphore_wait(barrier, along + slanted.astype(jnp.int32) + M)
    rounds = max(slices // 2 - 2, 0)

    def meet(index):
        if 0 < index <= rounds:
            pl.semaphore_wait(far.at[index - 1], along)
        if index < rounds:
            signal_along(far.at[index])
        if index == rounds:
            signal(far.at[rounds], partner, n)
        if index == rounds + 1:
            pl.semaphore_wait(far.at[rounds], 1)
            for step in range(1, M):
                signal(far.at[rounds + 1], p, lax.rem(n + step, M))
        if index == rounds + 2:
            pl.semaphore_wait(far.at[rounds + 1], M - 1)

    meet(0)
    for copy in loads:
        copy.wait()

    def shape_of(count):
        return prev3.at[:, pl.ds(0, count * LANE)]

    def remote(source, target, send, recv, tm, node):
        return pltpu.make_async_remote_copy(
            src_ref=source, dst_ref=target, send_sem=send, recv_sem=recv,
            device_id={"tm": tm, "node": node}, device_id_type=MESH,
        )

    def part(ref, c):
        begin = (bounds[c] + HALO if c else -HALO) + PAD
        end = bounds[c + 1] + HALO + PAD
        return ref.at[:, pl.ds(begin * LANE, (end - begin) * LANE)]

    def to_partner_own(c):
        return remote(part(own, c), part(prev1, c), s_prev1, r_prev1.at[c], partner, n)

    def to_partner_forward(c):
        return remote(part(prev2, c), part(prev1, c), s_prev1, r_prev1.at[c], partner, n)

    def slant_own(c):
        return remote(part(own, c), part(prev1, c), s_diag, r_prev1.at[c], slant, n)

    def ahead_own(c):
        return remote(part(own, c), part(prev2, c), s_prev2, r_prev2.at[c], ahead, n)

    def ahead_forward(c):
        return remote(part(prev1, c), part(prev3, c), s_prev3, r_prev3.at[c], ahead, n)

    def relay_forward(c):
        return remote(part(prev2, c), part(relay, c), s_relay, r_relay.at[c], ahead, n)

    def to_partner_relayed(c):
        return remote(part(relay, c), part(prev3, c), s_side, r_prev3.at[c], partner, n)

    def to_partner_second(c):
        return remote(part(prev2, c), part(prev3, c), s_side, r_prev3.at[c], partner, n)

    def relayed(c):
        return KINDS[c % len(KINDS)] == 0

    def crossed(c):
        return KINDS[c % len(KINDS)] != 2

    def sends_third(c):
        if relayed(c):
            return None
        if crossed(c):
            return jnp.logical_and(has_ahead, jnp.logical_and(even, has_behind))
        return jnp.logical_and(has_ahead, jnp.logical_not(first))

    def start_even(c):
        @pl.when(even)
        def _():
            to_partner_own(c).start()

            @pl.when(has_ahead)
            def _():
                ahead_own(c).start()

    def start_odd(c):
        @pl.when(jnp.logical_and(odd, has_ahead))
        def _():
            if c < SLANT:
                slant_own(c).start()
            ahead_own(c).start()

    def pass_across(c):
        @pl.when(has_behind)
        def _():
            ahead_own(c).wait_recv()

        @pl.when(jnp.logical_and(odd, has_behind))
        def _():
            if c >= SLANT:
                to_partner_forward(c).start()
            if relayed(c):

                @pl.when(has_ahead)
                def _():
                    relay_forward(c).start()

        if crossed(c):

            @pl.when(jnp.logical_and(even, has_behind))
            def _():
                to_partner_second(c).start()

    def pass_back(c):
        if relayed(c):

            @pl.when(jnp.logical_and(odd, p >= 5))
            def _():
                relay_forward(c).wait_recv()
                to_partner_relayed(c).start()

    def pass_ahead(c):
        @pl.when(odd)
        def _():
            to_partner_own(c).wait_recv()

        @pl.when(jnp.logical_and(even, has_behind))
        def _():
            to_partner_forward(c).wait_recv()

        if not relayed(c):

            @pl.when(sends_third(c))
            def _():
                ahead_forward(c).start()

    acc[...] = jnp.zeros_like(acc)

    def diffusion(v, c, k):
        size = (k + 2) * LANE
        right = pltpu.roll(v, size - 1, 1)
        flux = c * (right - v)
        left = pltpu.roll(flux, 1, 1)
        return (flux - left)[:, LANE:LANE + k * LANE]

    def finish(d, top, target, a):
        dd = d * d
        tt = top * top
        above = target * (d * dd) + (2.0 * a) * (top * tt)
        below = d * ((1.0 - a) * dd + (3.0 * a) * tt)
        guess = pl.reciprocal(below, approx=True)
        return above * (guess * (2.0 - below * guess))

    def two_steps(base, defect, u, square, reaction, a):
        d = (3.0 * a) * square + (1.0 - a)
        return finish(d, defect + u * d, base - a * reaction, a)

    def equal_nodes(begin, vw, cw, k):
        v = vw[:, LANE:LANE + k * LANE]
        square = v * v
        reaction = v - v * square
        four = 4.0 * (diffusion(vw, cw, k) + reaction)
        slope = 3.0 * square - 1.0
        lift = four + v * slope
        pull = four - reaction

        def node(m):
            a = implicit[m]
            return finish(1.0 + a * slope, begin + a * lift, begin + a * pull, a)

        return v, four, node

    def folded(value, k):
        out = value[:, :LANE]
        for piece in range(1, k):
            out = out + value[:, piece * LANE:(piece + 1) * LANE]
        return out

    def run(begin, end, block, counted):
        count = (end - begin) // STEP

        def step(i, carry):
            block(begin + i * STEP, STEP, counted)
            return carry

        lax.fori_loop(0, count, step, 0)
        if begin + count * STEP < end:
            block(begin + count * STEP, end - begin - count * STEP, counted)

    def over(c, lag, block):
        begin = bounds[c] + lag if c else 0
        end = min(bounds[c + 1] + lag, all_tiles)
        if c == 0 and lag:
            block(-lag, lag, False)
        run(begin, end, block, True)
        if c == chunks - 1 and lag:
            block(all_tiles, lag, False)

    def lanes(offset):
        return offset * LANE if isinstance(offset, int) else pl.multiple_of(offset * LANE, LANE)

    def wide(tile, k):
        return pl.ds(lanes(tile + PAD - 1), (k + 2) * LANE)

    def centre(tile, k):
        return pl.ds(lanes(tile + PAD), k * LANE)

    begun = {"even": 0, "odd": 0, "across": 0, "ahead": 0, "back": 0}
    moves = {
        "even": start_even, "odd": start_odd,
        "across": pass_across, "ahead": pass_ahead, "back": pass_back,
    }

    def proceed(name, upto):
        for index in range(begun[name], min(upto, chunks)):
            moves[name](index)
        begun[name] = max(begun[name], upto)

    for name, upto in START:
        proceed(name, upto)

    def stage(k, place):
        for name, upto in EARLY.get((k, place), ()):
            proceed(name, upto)
        if k >= SETTLED:
            for at, name, lead in STEADY:
                if at == place:
                    proceed(name, k + lead)

    def send_out(c):
        here_cells = pl.ds(bounds[c] * LANE, (bounds[c + 1] - bounds[c]) * LANE)
        target = out_hbm.at[0, 0, my_rows, here_cells]
        for step in (2, 3, 1):
            peer = lax.rem(n + step, M)
            remote(result.at[peer, :, here_cells], target, s_out, r_out, p, peer).start()
        pltpu.make_async_copy(result.at[n, :, here_cells], target, local_sem).start()

    for c in range(chunks):

        stage(c, 0)
        for name in moves:
            proceed(name, c + 1)

        @pl.when(p >= 3)
        def _():
            ahead_forward(c).wait_recv()

        def stage_a(tile, k, counted):
            middle = slice(LANE, LANE + k * LANE)
            cw = couple[:, wide(tile, k)]
            at = centre(tile, k)
            vw = own[:, wide(tile, k)]
            p1w = jnp.where(first, vw, prev1[:, wide(tile, k)])
            p1 = p1w[:, middle]
            p2w = jnp.where(p <= 1, p1w, prev2[:, wide(tile, k)])
            p2 = p2w[:, middle]
            p3 = jnp.where(p <= 2, p2, prev3[:, at])

            v, four, node = equal_nodes(p1, vw, cw, k)
            for m in range(M):
                here[m, :, at] = node(m)
            if counted:
                gap = p1 - v
                cross = 2.0 * sum(implicit)
                curve = sum(a * a for a in implicit)
                acc[0] += folded(
                    gap * (float(M) * gap + cross * four) + curve * (four * four), k
                )

            _, _, node = equal_nodes(p2, p1w, cw, k)
            for m in range(M):
                there[m, :, at] = node(m)

            _, _, node = equal_nodes(p3, p2w, cw, k)
            before[:, at] = jnp.where(second, p1, node(M - 1))

        over(c, 2, stage_a)
        stage(c, 1)

        def update(source, begin, cw, tile, k, which, counted):
            values = []
            forcings = []
            for m in range(M):
                vw = source[m, :, wide(tile, k)]
                v = vw[:, LANE:LANE + k * LANE]
                square = v * v
                reaction = v - v * square
                values.append((v, square, reaction))
                forcings.append(diffusion(vw, cw, k) + reaction)
            found = None
            outputs = []
            for m in range(M):
                base = begin
                for j in range(M):
                    base = base + weight[m][j] * forcings[j]
                v, square, reaction = values[m]
                defect = base - v
                if counted:
                    found = defect * defect if found is None else found + defect * defect
                outputs.append(two_steps(base, defect, v, square, reaction, implicit[m]))
            if counted:
                acc[which] += folded(found, k)
            return outputs

        def stage_b(tile, k, counted):
            cw = couple[:, wide(tile, k)]
            at = centre(tile, k)
            begin = jnp.where(first, own[:, centre(tile, k)], there[M - 1, :, at])
            outputs = update(here, begin, cw, tile, k, 1, counted)
            for m in range(M):
                mid[m, :, at] = outputs[m]
            mixed = None
            mixed_reaction = None
            for m in range(M):
                w = weight[M - 1][m]
                vw = there[m, :, wide(tile, k)]
                v = vw[:, LANE:LANE + k * LANE]
                square = v * v
                reaction = v - v * square
                mixed = w * vw if mixed is None else mixed + w * vw
                mixed_reaction = w * reaction if mixed_reaction is None else mixed_reaction + w * reaction
            base = before[:, at] + (diffusion(mixed, cw, k) + mixed_reaction)
            last = two_steps(base, base - v, v, square, reaction, implicit[M - 1])
            before[:, at] = jnp.where(first, own[:, centre(tile, k)], last)

        over(c, 1, stage_b)
        stage(c, 2)

        def stage_c(tile, k, counted):
            cw = couple[:, wide(tile, k)]
            outputs = update(mid, before[:, centre(tile, k)], cw, tile, k, 2, counted)
            at = pl.ds(lanes(tile), k * LANE)
            for m in range(M):
                result[m, :, at] = outputs[m]

        over(c, 0, stage_c)

        if c >= 2:
            meet(c - 1)
        if c + 1 < chunks:
            send_out(c)
        stage(c, 3)

    for index in range(max(chunks - 1, 1), rounds + 3):
        meet(index)
    lane = lax.broadcasted_iota(jnp.int32, (rows, LANE), 1)
    sub = lax.broadcasted_iota(jnp.int32, (rows, LANE), 0)
    mixed = jnp.zeros((rows, LANE), jnp.float32)
    for which in range(3):
        per_system = jnp.sum(acc[which], axis=1, keepdims=True)
        place = which * M * rows + n * rows + sub
        mixed = mixed + jnp.where(lane == place, per_system, 0.0)
    slot = p * M + n
    parts[slot] = jnp.sum(mixed, axis=0, keepdims=True)
    for other in range(slices - 1, -1, -1):
        for step in range(M - 1, -1, -1):
            if other or step:
                remote(
                    parts.at[slot], parts.at[slot], s_log, r_log,
                    lax.rem(p + other, slices), lax.rem(n + step, M),
                ).start()
    send_out(chunks - 1)
    others = parts.at[pl.ds(0, slices * M - 1)]
    gathered = remote(others, others, s_log, r_log, partner, n)
    gathered.wait_recv()
    summed = jnp.sum(parts[...], axis=0)
    logs = jnp.log(log_floor + summed / (slices * M * cells))
    for which in range(3):
        log_tile[which:which + 1, :] = logs[:, which * M * rows:(which + 1) * M * rows]
    log_copy = pltpu.make_async_copy(log_tile, log_ref, log_sem)
    log_copy.start()

    log_copy.wait()
    gathered.wait_send()
    three = result.at[pl.ds(0, M - 1)]
    outputs = remote(three, three, s_out, r_out, partner, n)
    outputs.wait_send()
    outputs.wait_recv()
    mine = result.at[0]
    pltpu.make_async_copy(mine, mine, local_sem).wait()

    def span(c):
        return bounds[c + 1] - bounds[c] + (0 if c else 2 * HALO)

    def drain(semaphore, wanted):
        count = sum(span(c) for c in range(chunks) if wanted(c))
        if count:
            remote(shape_of(count), shape_of(count), semaphore, r_prev3.at[0], partner, n).wait_send()

    def direct(c):
        return not relayed(c)

    def straight(c):
        return not crossed(c)

    @pl.when(has_ahead)
    def _():
        drain(s_prev2, lambda c: True)

    @pl.when(jnp.logical_and(has_ahead, jnp.logical_and(even, has_behind)))
    def _():
        drain(s_prev3, direct)

    @pl.when(jnp.logical_and(has_ahead, odd))
    def _():
        drain(s_prev3, straight)
        drain(s_diag, lambda c: c < SLANT)

    @pl.when(even)
    def _():
        drain(s_prev1, lambda c: True)

    @pl.when(jnp.logical_and(odd, has_behind))
    def _():
        drain(s_prev1, lambda c: c >= SLANT)

    @pl.when(jnp.logical_and(has_ahead, jnp.logical_and(odd, has_behind)))
    def _():
        drain(s_relay, relayed)

    @pl.when(jnp.logical_and(odd, p >= 5))
    def _():
        drain(s_side, relayed)

    @pl.when(jnp.logical_and(even, has_behind))
    def _():
        drain(s_side, crossed)


def unload(values, logs, values_hbm, logs_hbm, sem):
    size = values.shape[2] // PIECES
    copies = [pltpu.make_async_copy(logs, logs_hbm, sem.at[PIECES])]
    for piece in range(PIECES):
        at = pl.ds(piece * size, size)
        copies.append(
            pltpu.make_async_copy(values.at[:, :, at], values_hbm.at[:, :, at], sem.at[piece])
        )
    for copy in copies:
        copy.start()
    for copy in copies:
        copy.wait()


def solution(mesh):
    slices = mesh.shape["tm"]

    def body(slice_starts, coupling):
        systems, cells = coupling.shape
        rows = systems // M
        chunks = len(plan(cells // LANE)) - 1
        far = max(slices // 2 - 2, 0) + 2
        padded = cells + 2 * PAD * LANE
        f32 = jnp.float32
        dma = pltpu.SemaphoreType.DMA
        anyplace = pl.BlockSpec(memory_space=pl.ANY)
        anywhere = pl.BlockSpec(memory_space=pltpu.HBM)
        values, logs = pl.pallas_call(
            functools.partial(kernel, slices, rows, cells),
            out_shape=(
                jax.ShapeDtypeStruct((1, 1, systems, cells), f32),
                jax.ShapeDtypeStruct((3, systems), f32),
            ),
            in_specs=[anywhere, anywhere],
            out_specs=(anyplace, anyplace),
            scratch_shapes=[
                pltpu.VMEM((3, systems), f32), dma,
                pltpu.VMEM((rows, padded), f32),
                pltpu.VMEM((rows, padded), f32),
                pltpu.VMEM((rows, padded), f32),
                pltpu.VMEM((rows, padded), f32),
                pltpu.VMEM((rows, padded), f32),
                pltpu.VMEM((rows, padded), f32),
                pltpu.VMEM((M, rows, padded), f32),
                pltpu.VMEM((M, rows, padded), f32),
                pltpu.VMEM((M, rows, padded), f32),
                pltpu.VMEM((rows, padded), f32),
                pltpu.VMEM((M, rows, cells), f32),
                pltpu.VMEM((3, rows, LANE), f32),
                pltpu.VMEM((slices * M, 1, LANE), f32),
                dma((2,)),
                dma, dma((chunks,)), dma, dma((chunks,)), dma, dma((chunks,)),
                dma, dma((chunks,)), dma, dma, pltpu.SemaphoreType.REGULAR((far,)),
                dma, dma, dma, dma, dma,
            ],
            compiler_params=pltpu.CompilerParams(
                collective_id=0, has_side_effects=True, vmem_limit_bytes=48 * 1024 * 1024
            ),
        )(
            pltpu.with_memory_space_constraint(slice_starts, pltpu.HBM),
            pltpu.with_memory_space_constraint(coupling, pltpu.HBM),
        )
        return tuple(
            pl.pallas_call(
                unload,
                out_shape=(pltpu.HBM(values.shape, f32), pltpu.HBM(logs.shape, f32)),
                in_specs=[anyplace, anyplace],
                out_specs=(anywhere, anywhere),
                scratch_shapes=[dma((PIECES + 1,))],
                compiler_params=pltpu.CompilerParams(vmem_limit_bytes=1024 * 1024),
            )(values, logs)
        )

    return jax.shard_map(
        body,
        mesh=mesh,
        in_specs=(P("tm", None, None), P()),
        out_specs=(P("tm", "node", None, None), P()),
        check_vma=False,
    )
```
